768 devices in a mesh: pipe: 12 (over z), expert: 16 (over y, x_hi), tensor: 4 (over x_lo, core).
Axes of the slice: x: 4 (x_hi: 2, x_lo: 2; x = x_hi * 2 + x_lo), y: 8, z: 12, core: 2. Of those that a mesh axis runs over, the one named last changes fastest.
Arguments:
- inputs_prev: bfloat16 [12, 2048, 3584], P('pipe', 'expert', 'tensor'), may hold values from -6 to 6
- cotangent_next: bfloat16 [12, 2048, 3584], P('pipe', 'expert', 'tensor'), may hold values from -6 to 6
- saved_input: bfloat16 [12, 2048, 3584], P('pipe', 'expert', 'tensor'), may hold values from -6 to 6
- expert_ids: int32 [2, 12, 2048, 8], P(None, 'pipe', 'expert'), may hold values from 0 to 255, as said below
- keep_mask: int32 [2, 12, 2048, 8], P(None, 'pipe', 'expert'), may hold values from 0 to 1, as said below
- slot_pos: int32 [2, 12, 2048, 8], P(None, 'pipe', 'expert'), may hold values from 0 to 3, as said below
- weight_q: int32 [2, 12, 2048, 8], P(None, 'pipe', 'expert'), may hold values from 1 to 4095
- gate_routed: bfloat16 [12, 16, 3584, 512], P('pipe', 'expert', None, 'tensor'), may hold values from -0.09375 to 0.09375
- up_routed: bfloat16 [12, 16, 3584, 512], P('pipe', 'expert', None, 'tensor'), may hold values from -0.09375 to 0.09375
- down_routed: bfloat16 [12, 16, 512, 3584], P('pipe', 'expert', 'tensor'), may hold values from -0.1875 to 0.1875
- gate_shared: bfloat16 [12, 3584, 1024], P('pipe', None, 'tensor'), may hold values from -0.09375 to 0.09375
- up_shared: bfloat16 [12, 3584, 1024], P('pipe', None, 'tensor'), may hold values from -0.09375 to 0.09375
- down_shared: bfloat16 [12, 1024, 3584], P('pipe', 'tensor'), may hold values from -0.1875 to 0.1875
Outputs:
- out_act: bfloat16 [12, 2048, 3584], P('pipe', 'expert', 'tensor')
- in_grad: bfloat16 [12, 2048, 3584], P('pipe', 'expert', 'tensor')
The draws below stay inside these ranges and needn't reach their ends.
Inputs may be any that keep to these rules, and one draw needn't show every extreme that they name: `expert_ids`: each row names 8 different experts; in every section and micro-batch one expert below 8 is named by every row. `keep_mask`: 1 only where the expert named is below 8; in one block of 128 rows no expert has more than 4 kept choices, and in every section and micro-batch one expert has exactly 4 in every block. `slot_pos`: kept choices of one block naming the same expert hold different slots; 0 where keep_mask is 0.
All inputs are finite; a program needn't handle non-finite values.
Results may differ from the reference program's by a relative error of at most 0.005.
Values may be sent and summed in bfloat16 or wider, within the bound.
No kernel may reach another device: no remote copies, remote signals or barrier semaphores. Data moves between devices by JAX's collectives and lax.ppermute only.
A program may use at most 64 MiB of HBM per device.

```python
import jax
import jax.numpy as jnp
from jax import lax

D = 3584
FE = 1024
FS = 1024
SPECIALIST_COUNT = 256
TOPK = 8
TOK_DEV = 128
SECTIONS = 12
EXPERTS = 8
TOKENS = 2048
CAP = 4
N_EXPERT = 16
N_TENSOR = 4


def routing_tables(key):
    base = jax.random.fold_in(key, 29)
    key_score, key_lean, key_force, key_order = jax.random.split(base, 4)
    blocks = TOKENS // TOK_DEV
    choices = TOK_DEV * TOPK
    gating_logits = jax.random.randint(key_score, (2, SECTIONS, TOKENS, SPECIALIST_COUNT), 0, 65536)
    preference_offset = jax.random.randint(key_lean, (SPECIALIST_COUNT,), 0, 3) * 32768
    imposed_selection = jax.random.randint(key_force, (2, SECTIONS, 1, 1), 0, EXPERTS)
    uniform_draws = jnp.arange(SPECIALIST_COUNT, dtype=jnp.int32)
    extra_increment = jnp.where(uniform_draws == imposed_selection, 1 << 20, 0)
    sorted_specialists = (gating_logits + preference_offset + extra_increment) * SPECIALIST_COUNT + uniform_draws
    _, chosen = lax.top_k(sorted_specialists, TOPK)
    chosen = chosen.astype(jnp.int32)
    lined = chosen.reshape(2 * SECTIONS * blocks, choices)
    onehot = (lined[:, :, None] == jnp.arange(EXPERTS, dtype=jnp.int32)).astype(jnp.int32)
    order_keys = jax.random.split(key_order, 2 * SECTIONS * blocks)
    order = jax.vmap(lambda single: jax.random.permutation(single, choices))(order_keys).astype(jnp.int32)
    placed = jnp.take_along_axis(onehot, order[:, :, None], axis=1)
    before = jnp.cumsum(placed, axis=1) - placed
    rank_sorted = jnp.sum(before * placed, axis=-1)
    inverse = jnp.argsort(order, axis=1, stable=True)
    position = jnp.take_along_axis(rank_sorted, inverse, axis=1)
    kept = (lined < EXPERTS) & (position < CAP)
    slots = jnp.where(kept, position, 0)
    target_shape = (2, SECTIONS, TOKENS, TOPK)
    return (chosen, kept.astype(jnp.int32).reshape(target_shape), slots.astype(jnp.int32).reshape(target_shape))


def draw_expert_ids(key, part):
    return routing_tables(key)[0]


def draw_keep_mask(key, part):
    return routing_tables(key)[1]


def draw_slot_pos(key, part):
    return routing_tables(key)[2]


def with_ends(drawn, own_key, low, largest):
    place = [jax.random.randint(jax.random.fold_in(own_key, axis), (), 0, length) for axis, length in enumerate(drawn.shape)]
    main_axis = drawn.shape.index(max(drawn.shape))
    next_to = place[:main_axis] + [(place[main_axis] + 1) % drawn.shape[main_axis]] + place[main_axis + 1:]
    return drawn.at[tuple(place)].set(low).at[tuple(next_to)].set(largest)


def block_scale(stream_key, extent, cuts, smallest, top_value):
    factor_of = 1.0
    for axis_at, blocks in cuts:
        draws = jax.random.uniform(jax.random.fold_in(jax.random.fold_in(stream_key, 6), axis_at), (blocks,), jnp.float32, smallest / len(cuts), top_value / len(cuts))
        factor_of = factor_of * jnp.repeat(jnp.exp(draws), extent[axis_at] // blocks).reshape((-1,) + (1,) * (len(extent) - 1 - axis_at))
    return factor_of


def scatter_about(own_key, dims, width, bound, shards=(), kind=jnp.bfloat16):
    drawn = jax.random.normal(own_key, dims, jnp.float32) * width
    if len(shards) > 0:
        drawn = block_scale(own_key, dims, shards, -0.22, 0.18) * drawn
    return jnp.clip(drawn, min=-bound, max=bound).astype(kind)


def setup_inputs(seed: int = 0) -> dict:
    key_of = jax.random.split(jax.random.key(seed), 14)
    return {
        "inputs_prev": scatter_about(key_of[0], (SECTIONS, TOKENS, D), 1.0, 6.0, ((0, 12), (1, 16), (2, 4))),
        "cotangent_next": scatter_about(key_of[1], (SECTIONS, TOKENS, D), 1.0, 6.0, ((0, 12), (1, 16), (2, 4))),
        "saved_input": scatter_about(key_of[2], (SECTIONS, TOKENS, D), 1.0, 6.0, ((0, 12), (1, 16), (2, 4))),
        "expert_ids": draw_expert_ids(jax.random.fold_in(key_of[13], 71), 0),
        "keep_mask": draw_keep_mask(jax.random.fold_in(key_of[13], 71), 0),
        "slot_pos": draw_slot_pos(jax.random.fold_in(key_of[13], 71), 0),
        "weight_q": with_ends(jax.random.randint(key_of[6], (2, SECTIONS, TOKENS, TOPK), 1, 4096), jax.random.fold_in(key_of[6], 1), 1, 4095).astype(jnp.int32),
        "gate_routed": scatter_about(key_of[7], (SECTIONS, N_EXPERT, D, FE // 2), D ** -0.5, 0.09375, ((0, 12), (1, 16), (3, 4))),
        "up_routed": scatter_about(key_of[8], (SECTIONS, N_EXPERT, D, FE // 2), D ** -0.5, 0.09375, ((0, 12), (1, 16), (3, 4))),
        "down_routed": scatter_about(key_of[9], (SECTIONS, N_EXPERT, FE // 2, D), FE ** -0.5, 0.1875, ((0, 12), (1, 16), (2, 4))),
        "gate_shared": scatter_about(key_of[10], (SECTIONS, D, FS), D ** -0.5, 0.09375, ((0, 12), (2, 4))),
        "up_shared": scatter_about(key_of[11], (SECTIONS, D, FS), D ** -0.5, 0.09375, ((0, 12), (2, 4))),
        "down_shared": scatter_about(key_of[12], (SECTIONS, FS, D), FS ** -0.5, 0.1875, ((0, 12), (1, 4))),
    }


def swish(values):
    return values * jax.nn.sigmoid(values)


def swish_slope(values):
    logistic = jax.nn.sigmoid(values)
    return logistic * (1.0 + values * (1.0 - logistic))


def slot_plan(choice_ids, kept_flags, slot_index, weight_levels, experts_here, capacity):
    total_slots = experts_here * capacity
    target = jnp.where(kept_flags > 0, choice_ids * capacity + slot_index, total_slots).reshape(-1).astype(jnp.int32)
    source = jnp.broadcast_to(jnp.arange(choice_ids.shape[0], dtype=jnp.int32)[:, None], choice_ids.shape).reshape(-1)
    slot_token = jnp.zeros((total_slots,), jnp.int32).at[target].set(source, mode="drop")
    levels = (weight_levels.astype(jnp.float32) / 4096.0).reshape(-1)
    slot_weight = jnp.zeros((total_slots,), jnp.float32).at[target].set(levels, mode="drop")
    slot_live = jnp.zeros((total_slots,), jnp.float32).at[target].set(1.0, mode="drop")
    return slot_token, slot_weight, slot_live


def contract_last(left, right):
    return lax.dot_general(left, right, (((1,), (1,)), ((), ())), preferred_element_type=jnp.float32)


def expert_pass(packed):
    rows_in, rows_saved, rows_cot, gate_w, up_w, down_w = packed
    part_width = FE // (2 * N_TENSOR)
    gate_pre = jnp.dot(rows_in, gate_w, preferred_element_type=jnp.float32)
    up_pre = jnp.dot(rows_in, up_w, preferred_element_type=jnp.float32)
    hidden = (swish(gate_pre) * up_pre).astype(jnp.bfloat16)
    gate_back = jnp.dot(rows_saved, gate_w, preferred_element_type=jnp.float32)
    up_back = jnp.dot(rows_saved, up_w, preferred_element_type=jnp.float32)
    grad_hidden = contract_last(rows_cot, down_w)
    grad_gate = (grad_hidden * up_back * swish_slope(gate_back)).astype(jnp.bfloat16)
    grad_up = (grad_hidden * swish(gate_back)).astype(jnp.bfloat16)
    result = jnp.zeros((rows_in.shape[0], rows_in.shape[1]), jnp.float32)
    grad_rows = jnp.zeros((rows_in.shape[0], rows_in.shape[1]), jnp.float32)
    for group_j in range(FE // part_width):
        lower = group_j * part_width
        upper = lower + part_width
        piece_out = jnp.dot(hidden[:, lower:upper], down_w[lower:upper], preferred_element_type=jnp.float32)
        result = result + piece_out.astype(jnp.bfloat16).astype(jnp.float32)
        piece_grad = contract_last(grad_gate[:, lower:upper], gate_w[:, lower:upper]) + contract_last(grad_up[:, lower:upper], up_w[:, lower:upper])
        grad_rows = grad_rows + piece_grad.astype(jnp.bfloat16).astype(jnp.float32)
    return result, grad_rows


def shared_pass(full_in, full_saved, full_cot, gate_w, up_w, down_w):
    gate_pre = jnp.dot(full_in, gate_w, preferred_element_type=jnp.float32)
    up_pre = jnp.dot(full_in, up_w, preferred_element_type=jnp.float32)
    hidden = (swish(gate_pre) * up_pre).astype(jnp.bfloat16)
    shared_out = jnp.dot(hidden, down_w, preferred_element_type=jnp.float32)
    gate_back = jnp.dot(full_saved, gate_w, preferred_element_type=jnp.float32)
    up_back = jnp.dot(full_saved, up_w, preferred_element_type=jnp.float32)
    grad_hidden = contract_last(full_cot, down_w)
    grad_gate = (grad_hidden * up_back * swish_slope(gate_back)).astype(jnp.bfloat16)
    grad_up = (grad_hidden * swish(gate_back)).astype(jnp.bfloat16)
    shared_grad = contract_last(grad_gate, gate_w) + contract_last(grad_up, up_w)
    return shared_out, shared_grad


def one_section(packed):
    (section_in, section_saved, section_cot, ids_fwd, keep_fwd, slot_fwd, level_fwd, ids_bwd, keep_bwd, slot_bwd, level_bwd,
     gate_section, up_section, down_section, shared_gate, shared_up, shared_down) = packed
    blocks = TOKENS // TOK_DEV
    half_width = FE // 2

    def plan_all(ids_all, keep_all, slot_all, level_all):
        return jax.vmap(lambda a, b, c, e: slot_plan(a, b, c, e, EXPERTS, CAP))(
            ids_all.reshape(blocks, TOK_DEV, TOPK), keep_all.reshape(blocks, TOK_DEV, TOPK),
            slot_all.reshape(blocks, TOK_DEV, TOPK), level_all.reshape(blocks, TOK_DEV, TOPK))

    token_f, weight_f, live_f = plan_all(ids_fwd, keep_fwd, slot_fwd, level_fwd)
    token_b, weight_b, live_b = plan_all(ids_bwd, keep_bwd, slot_bwd, level_bwd)

    def pick(values, tokens_at, live_at):
        return jnp.where(live_at[:, None] > 0, values[tokens_at], jnp.zeros((), values.dtype))

    def scaled(values, tokens_at, weight_at):
        return (weight_at[:, None] * values[tokens_at].astype(jnp.float32)).astype(jnp.bfloat16)

    rows_in = jax.vmap(pick)(section_in.reshape(blocks, TOK_DEV, D), token_f, live_f)
    rows_saved = jax.vmap(pick)(section_saved.reshape(blocks, TOK_DEV, D), token_b, live_b)
    rows_cot = jax.vmap(scaled)(section_cot.reshape(blocks, TOK_DEV, D), token_b, weight_b)

    def to_expert(rows):
        return rows.reshape(blocks, EXPERTS, CAP, D).transpose(1, 0, 2, 3).reshape(EXPERTS, blocks * CAP, D)

    def from_expert(rows):
        return rows.reshape(EXPERTS, blocks, CAP, D).transpose(1, 0, 2, 3).reshape(blocks, EXPERTS * CAP, D)

    gate_full = gate_section.reshape(EXPERTS, 2, D, half_width).transpose(0, 2, 1, 3).reshape(EXPERTS, D, FE)
    up_full = up_section.reshape(EXPERTS, 2, D, half_width).transpose(0, 2, 1, 3).reshape(EXPERTS, D, FE)
    down_full = down_section.reshape(EXPERTS, FE, D)
    expert_out, expert_grad = lax.map(expert_pass, (to_expert(rows_in), to_expert(rows_saved), to_expert(rows_cot), gate_full, up_full, down_full))

    def combine(tokens_at, weight_at, rows):
        return jnp.zeros((TOK_DEV, D), jnp.float32).at[tokens_at].add(weight_at[:, None] * rows)

    routed_out = jax.vmap(combine)(token_f, weight_f, from_expert(expert_out)).reshape(TOKENS, D)
    routed_grad = jax.vmap(combine)(token_b, live_b, from_expert(expert_grad)).reshape(TOKENS, D)
    shared_out, shared_grad = shared_pass(section_in, section_saved, section_cot, shared_gate, shared_up, shared_down)
    return (shared_out + routed_out).astype(jnp.bfloat16), (shared_grad + routed_grad).astype(jnp.bfloat16)


def reference(inputs_prev, cotangent_next, saved_input, expert_ids, keep_mask, slot_pos, weight_q, gate_routed, up_routed, down_routed, gate_shared, up_shared, down_shared):
    forward_in = jnp.roll(inputs_prev, 1, axis=0)
    backward_in = jnp.roll(cotangent_next, -1, axis=0)
    out_act, in_grad = lax.map(one_section, (forward_in, saved_input, backward_in,
                                           expert_ids[0], keep_mask[0], slot_pos[0], weight_q[0],
                                           expert_ids[1], keep_mask[1], slot_pos[1], weight_q[1],
                                           gate_routed, up_routed, down_routed, gate_shared, up_shared, down_shared))
    return out_act, in_grad
```

```python
import jax
import jax.numpy as jnp
from jax import lax
from jax.sharding import Mesh, PartitionSpec as P

BF = jnp.bfloat16
F32 = jnp.float32
CAP = 4
RING = ("xh", "xl", "core")


def shifted(block, axis, distance):
    n = lax.axis_size(axis)
    return lax.ppermute(block, axis, [((i - distance) % n, i) for i in range(n)])


def swish_and_slope(v):
    s = jax.nn.sigmoid(v)
    return v * s, s * (1.0 + v * (1.0 - s))


def dot(a, b):
    return jnp.dot(a, b, preferred_element_type=F32)


def contract_last(left, right):
    return lax.dot_general(left, right, (((1,), (1,)), ((), ())), preferred_element_type=F32)


def slot_select(ids, keep, slot, weight_q, slots):
    target = jnp.where(keep > 0, ids * CAP + slot, slots).T
    hit = target[None] == lax.broadcasted_iota(jnp.int32, (slots, 1, 1), 0)
    weight = (weight_q.astype(F32) / 4096.0).T
    one = jnp.sum(jnp.where(hit, 1.0, 0.0), axis=1)
    return one, jnp.sum(jnp.where(hit, weight[None], 0.0), axis=1)


def spread(block, axis):
    return lax.all_to_all(jnp.broadcast_to(block[None], (2, *block.shape)), axis, 0, 0, tiled=True)


def local(inputs_prev, cotangent_next, saved_input, expert_ids, keep_mask, slot_pos, weight_q,
          gate_routed, up_routed, down_routed, gate_shared, up_shared, down_shared):
    tokens, shard = inputs_prev.shape[1:]
    experts = lax.axis_size("y")
    slots = experts * CAP
    saved = saved_input[0]
    fwd = shifted(inputs_prev[0], "pipe", 1)
    cot = shifted(cotangent_next[0], "pipe", -1)
    one_f, w_f = slot_select(expert_ids[0, 0], keep_mask[0, 0], slot_pos[0, 0], weight_q[0, 0], slots)
    one_b, w_b = slot_select(expert_ids[1, 0], keep_mask[1, 0], slot_pos[1, 0], weight_q[1, 0], slots)

    rows_f = dot(one_f.astype(BF), fwd).astype(BF)
    rows_s = dot(one_b.astype(BF), saved).astype(BF)
    rows_c = (jnp.sum(w_b, axis=1, keepdims=True) * dot(one_b.astype(BF), cot)).astype(BF)
    parcel = jnp.stack([r.reshape(experts, CAP, shard) for r in (rows_f, rows_s, rows_c)], axis=1)
    parcel = lax.all_to_all(parcel, "y", 0, 0, tiled=True)
    parcel = parcel.transpose(1, 0, 2, 3).reshape(3 * slots, shard)
    ring = lax.axis_size("xh") * 4
    got = lax.all_to_all(jnp.broadcast_to(parcel[None], (ring, *parcel.shape)), RING, 0, 0, tiled=True)
    got = got.reshape(2, 4, 3, slots, shard).transpose(2, 0, 3, 1, 4).reshape(3, 2 * slots, 4 * shard)

    def full(v):
        a = spread(v, "xl")
        b = spread(a, "core")
        return b.transpose(2, 1, 0, 3).reshape(tokens, 4 * shard)

    full_s = full(saved)
    full_f = full(fwd)
    full_c = full(cot)

    def compute(x, s, c, gate, up, down):
        n = x.shape[0]
        both = jnp.concatenate([x, s], axis=0)
        a = dot(both, gate)
        b = dot(both, up)
        dh = contract_last(c, down)
        act, slope = swish_and_slope(a)
        hidden = (act[:n] * b[:n]).astype(BF)
        gg = (dh * b[n:] * slope[n:]).astype(BF)
        gu = (dh * act[n:]).astype(BF)
        out = dot(hidden, down).astype(BF)
        grad = (contract_last(gg, gate) + contract_last(gu, up)).astype(BF)
        return out, grad

    out_r, grad_r = compute(got[0], got[1], got[2], gate_routed[0, 0], up_routed[0, 0], down_routed[0, 0])
    both = jnp.stack([out_r, grad_r]).reshape(2, 2, slots, 4, shard).transpose(1, 3, 0, 2, 4)
    both = lax.all_to_all(both.reshape(ring, 2 * slots, shard), RING, 0, 0, tiled=True)
    both = jnp.sum(both.astype(F32), axis=0).reshape(2, experts, CAP, shard).transpose(1, 0, 2, 3)
    both = lax.all_to_all(both.astype(BF), "y", 0, 0, tiled=True)
    both = both.transpose(1, 0, 2, 3).reshape(2, slots, shard).astype(F32)

    out_s, grad_s = compute(full_f, full_s, full_c, gate_shared[0], up_shared[0], down_shared[0])
    part = jnp.stack([out_s, grad_s]).reshape(2, tokens, 2, 2, shard).transpose(3, 2, 0, 1, 4)
    part = lax.all_to_all(part, "core", 0, 0, tiled=True)
    part = (part[0].astype(F32) + part[1].astype(F32)).astype(BF)
    part = lax.all_to_all(part, "xl", 0, 0, tiled=True)
    part = part[0].astype(F32) + part[1].astype(F32)

    def merge(weights, rows):
        return lax.dot_general(weights, rows, (((0,), (0,)), ((), ())), precision=lax.Precision.HIGHEST,
                               preferred_element_type=F32)

    out = part[0] + merge(w_f, both[0])
    grad = part[1] + merge(one_b, both[1])
    return out.astype(BF)[None], grad.astype(BF)[None]


def solution(mesh):
    pipe, expert, tensor = mesh.devices.shape
    fine = Mesh(mesh.devices.reshape(pipe, expert // 2, 2, 2, tensor // 2), ("pipe", "y", "xh", "xl", "core"))
    e, t = ("y", "xh"), ("xl", "core")
    act = P("pipe", e, t)
    table = P(None, "pipe", e, None)
    return jax.shard_map(
        local,
        mesh=fine,
        in_specs=(act, act, act, table, table, table, table,
                  P("pipe", e, None, t), P("pipe", e, None, t), P("pipe", e, t, None),
                  P("pipe", None, t), P("pipe", None, t), P("pipe", t, None)),
        out_specs=(act, act),
        check_vma=False,
    )
```

```python
import functools

import jax
import jax.numpy as jnp
from jax import lax
from jax.experimental import pallas as pl
from jax.experimental.pallas import tpu as pltpu
from jax.sharding import Mesh, PartitionSpec as P

BF = jnp.bfloat16
F32 = jnp.float32
I32 = jnp.int32
CAP = 4
PAD = 4 * CAP


def call(body, name, outs, grid=(1,), in_specs=None, out_specs=None, scratch=(), flops=0):
    spec = pltpu.PrefetchScalarGridSpec(
        num_scalar_prefetch=1, grid=grid, in_specs=in_specs, out_specs=out_specs, scratch_shapes=scratch
    )
    return pl.pallas_call(
        body, grid_spec=spec, out_shape=outs, name=name,
        cost_estimate=pl.CostEstimate(flops=flops, transcendentals=0, bytes_accessed=0),
        compiler_params=pltpu.CompilerParams(vmem_limit_bytes=48 * 2**20),
    )


def whole(shape):
    return pl.BlockSpec(shape, lambda j, s: (0,) * len(shape))


def shape_of(dtype, *dims):
    return jax.ShapeDtypeStruct(dims, dtype)


def shifted(block, axis, distance):
    n = lax.axis_size(axis)
    return lax.ppermute(block, axis, [((i - distance) % n, i) for i in range(n)])


def swapped(block, axis):
    return lax.ppermute(block, axis, [(0, 1), (1, 0)])


def dot(a, b):
    return jnp.dot(a, b, preferred_element_type=F32)


def contract_last(left, right):
    return lax.dot_general(left, right, (((1,), (1,)), ((), ())), preferred_element_type=F32)


def tables_body(s, ids, keep, slot, wq, sel_f, sel_s, sel_c, scale, add_hi, add_lo, add_b):
    tokens = ids.shape[2]
    row = lax.broadcasted_iota(I32, (tokens, 1), 0)
    arr = (row // CAP) % 4
    slot_id = (row // PAD) * CAP + row % CAP
    back = 8 * (tokens // PAD)
    row2 = lax.broadcasted_iota(I32, (back, 1), 0)
    dirn = (row2 // CAP) % 2
    slot2 = (row2 // 8) * CAP + row2 % CAP
    want_f = jnp.where(arr == 0, slot_id, -1)
    want_b = jnp.where((arr == 1) | (arr == 2), slot_id, -1)
    back_f = jnp.where(dirn == 0, slot2, -1)
    back_b = jnp.where(dirn == 1, slot2, -1)
    hit_f = jnp.zeros((tokens, tokens), F32)
    hit_b = jnp.zeros((tokens, tokens), F32)
    weight = jnp.zeros((tokens, tokens), F32)
    hi = jnp.zeros((back, tokens), F32)
    lo = jnp.zeros((back, tokens), F32)
    one = jnp.zeros((back, tokens), F32)
    target = jnp.where(keep[...] > 0, ids[...] * CAP + slot[...], -2)
    level = wq[...]
    for k in range(ids.shape[1]):
        tf = target[0, k : k + 1]
        tb = target[1, k : k + 1]
        lf = level[0, k : k + 1]
        lb = level[1, k : k + 1].astype(F32) * (1.0 / 4096.0)
        top = (lf // 64) * 64
        hit_f += jnp.where(tf == want_f, 1.0, 0.0)
        eq = tb == want_b
        hit_b += jnp.where(eq, 1.0, 0.0)
        weight += jnp.where(eq, lb, 0.0)
        eq = tf == back_f
        hi += jnp.where(eq, top.astype(F32) * (1.0 / 4096.0), 0.0)
        lo += jnp.where(eq, (lf - top).astype(F32) * (1.0 / 4096.0), 0.0)
        one += jnp.where(tb == back_b, 1.0, 0.0)
    sel_f[...] = hit_f.astype(BF)
    sel_s[...] = jnp.where(arr == 1, hit_b, 0.0).astype(BF)
    sel_c[...] = jnp.where(arr == 2, hit_b, 0.0).astype(BF)
    scale[...] = jnp.sum(weight, axis=1, keepdims=True)
    add_hi[...] = hi.T.astype(BF)
    add_lo[...] = lo.T.astype(BF)
    add_b[...] = one.T.astype(BF)


def parcel_body(s, sel_f, sel_s, sel_c, scale, fwd, saved, cot, out):
    rows = dot(sel_f[...], fwd[...]) + dot(sel_s[...], saved[...]) + scale[...] * dot(sel_c[...], cot[...])
    out[...] = rows.astype(BF)


def fan_body(s, got, out):
    n = got.shape[0]
    m = n * 3 // 4
    half = n // 2
    r = lax.broadcasted_iota(I32, (m, n), 0)
    c = lax.broadcasted_iota(I32, (m, n), 1)
    k = r - half
    source = jnp.where(r < half, (r // 8) * PAD + r % 8, (k // CAP) * PAD + 8 + k % CAP)
    rows = dot(jnp.where(c == source, 1.0, 0.0).astype(BF), got[...]).astype(BF)
    for i in range(out.shape[0]):
        out[i] = rows


def pack_body(s, gs, us, gr, ur, ds, dr, in_side, out_side):
    w = gs.shape[2]
    n = gr.shape[2]
    in_side[:, 0:w] = gs[0]
    in_side[:, w : 2 * w] = us[0]
    in_side[:, 2 * w : 2 * w + n] = gr[0]
    in_side[:, 2 * w + n : 2 * w + 2 * n] = ur[0]
    out_side[0 : ds.shape[0]] = ds[...]
    out_side[ds.shape[0] :] = dr[...]


def pre(acc, first, both, cot, gate, up, down, gate_o, up_o, down_o):
    n = both.shape[0]
    m = cot.shape[0]
    w = gate.shape[1]

    def put(r0, r1, c0, c1, v):
        @pl.when(first)
        def _():
            acc[r0:r1, c0:c1] = v

        @pl.when(jnp.logical_not(first))
        def _():
            acc[r0:r1, c0:c1] += v

    put(0, n, 0, w, dot(both, gate))
    put(0, n, w, 2 * w, dot(both, gate_o))
    put(n, 2 * n, 0, w, dot(both, up))
    put(n, 2 * n, w, 2 * w, dot(both, up_o))
    put(2 * n, 2 * n + m, 0, w, contract_last(cot, down))
    put(2 * n, 2 * n + m, w, 2 * w, contract_last(cot, down_o))


def joined(mine, other):
    w = mine.shape[1] // 2
    return jnp.concatenate([mine[:, :w] + other[:, w:], mine[:, w:] + other[:, :w]], axis=1)


def shared_pre_body(s, own_f, own_s, own_c, far_f, far_s, far_c, gate, up, down, gate_o, up_o, down_o, acc):
    j = pl.program_id(0)
    near = j == 0
    both = jnp.concatenate(
        [jnp.where(near, own_f[...], far_f[...]), jnp.where(near, own_s[...], far_s[...])], axis=0
    )
    cot = jnp.where(near, own_c[...], far_c[...])
    pre(acc, near, both, cot, gate[0], up[0], down[...], gate_o[...], up_o[...], down_o[...])


def shared_post_body(s, mine, other, gate, up, down, gate_o, up_o, down_o, send, keep, hid, gg, gu):
    j = pl.program_id(0)
    n = hid.shape[0]
    w = gate.shape[2]

    @pl.when(j == 0)
    def _():
        a_f = joined(mine[0:n], other[0:n])
        a_s = joined(mine[n : 2 * n], other[n : 2 * n])
        b_f = joined(mine[2 * n : 3 * n], other[2 * n : 3 * n])
        b_s = joined(mine[3 * n : 4 * n], other[3 * n : 4 * n])
        dh = joined(mine[4 * n : 5 * n], other[4 * n : 5 * n])
        hid[...] = (a_f * jax.nn.sigmoid(a_f) * b_f).astype(BF)
        sg = jax.nn.sigmoid(a_s)
        gg[...] = (dh * b_s * (sg * (1.0 + a_s * (1.0 - sg)))).astype(BF)
        gu[...] = (dh * (a_s * sg)).astype(BF)

    out = dot(hid[:, :w], down[...]) + dot(hid[:, w:], down_o[...])
    grad = (
        contract_last(gg[:, :w], gate[0]) + contract_last(gg[:, w:], gate_o[...])
        + contract_last(gu[:, :w], up[0]) + contract_last(gu[:, w:], up_o[...])
    )

    @pl.when(j == 0)
    def _():
        send[0] = out.astype(BF)
        send[1] = grad.astype(BF)

    @pl.when(j == 1)
    def _():
        keep[0] = out
        keep[1] = grad


def expert_pre_body(s, got, gate, up, down, gate_o, up_o, down_o, acc):
    j = pl.program_id(0)
    half = got.shape[2] * 2 // 3
    both = jnp.concatenate([got[0, 0, :half], got[1, 0, :half]], axis=0)
    cot = jnp.concatenate([got[0, 0, half:], got[1, 0, half:]], axis=0)
    pre(acc, j == 0, both, cot, gate[0], up[0], down[...], gate_o[...], up_o[...], down_o[...])


def expert_post_body(s, mine, other, gate, up, down, gate_o, up_o, down_o, out, hid, gg, gu):
    j = pl.program_id(0)
    n = hid.shape[0]
    m = n // 2
    w = gate.shape[2]

    @pl.when(j == 0)
    def _():
        a = joined(mine[0:n], other[0:n])
        b = joined(mine[n : 2 * n], other[n : 2 * n])
        dh = joined(mine[2 * n : 2 * n + m], other[2 * n : 2 * n + m])
        r = lax.broadcasted_iota(I32, (n, m), 0)
        c = lax.broadcasted_iota(I32, (n, m), 1)
        place = jnp.where(c == (r // 8) * CAP + r % CAP, 1.0, 0.0)
        dh = jnp.dot(place, dh, precision=lax.Precision.HIGHEST, preferred_element_type=F32)
        back = (lax.broadcasted_iota(I32, (n, 1), 0) // CAP) % 2 == 1
        sg = jax.nn.sigmoid(a)
        hid[...] = jnp.where(back, 0.0, a * sg * b).astype(BF)
        gg[...] = jnp.where(back, dh * b * (sg * (1.0 + a * (1.0 - sg))), 0.0).astype(BF)
        gu[...] = jnp.where(back, dh * (a * sg), 0.0).astype(BF)

    rows = (
        dot(hid[:, :w], down[...]) + dot(hid[:, w:], down_o[...])
        + contract_last(gg[:, :w], gate[0]) + contract_last(gg[:, w:], gate_o[...])
        + contract_last(gu[:, :w], up[0]) + contract_last(gu[:, w:], up_o[...])
    ).astype(BF)
    out[0, 0] = rows[:m]
    out[1, 0] = rows[m:]


def merge_body(s, back, keep, far, add_hi, add_lo, add_b, out, grad):
    rows = back[...]
    out[...] = (keep[0] + far[0].astype(F32) + (dot(add_hi[...], rows) + dot(add_lo[...], rows))).astype(BF)
    grad[...] = (keep[1] + far[1].astype(F32) + dot(add_b[...], rows)).astype(BF)


def local(inputs_prev, cotangent_next, saved_input, expert_ids, keep_mask, slot_pos, weight_q,
          gate_routed, up_routed, down_routed, gate_shared, up_shared, down_shared):
    tokens, shard = inputs_prev.shape[1:]
    experts = lax.axis_size("y")
    here = jnp.stack([lax.axis_index("xl"), lax.axis_index("core")]).astype(I32)
    saved = saved_input[0]
    gs = gate_shared[0].reshape(4, shard, -1)
    us = up_shared[0].reshape(4, shard, -1)
    ds = down_shared[0]
    gr = gate_routed[0, 0].reshape(4, shard, -1)
    ur = up_routed[0, 0].reshape(4, shard, -1)
    dr = down_routed[0, 0]
    fs = gs.shape[2]
    fe = gr.shape[2]

    fwd = shifted(inputs_prev[0], "pipe", 1)
    cot = shifted(cotangent_next[0], "pipe", -1)
    far_s = swapped(saved, "xl")

    def rows_at(n, which):
        return pl.BlockSpec((1, shard, n), lambda j, s: (which(j, s), 0, 0))

    def cols_at(n, which):
        return pl.BlockSpec((n, shard), lambda j, s: (0, which(j, s)))

    theirs = lambda j, s: 2 * j + 1 - s[1]
    in_side, out_side = call(
        pack_body, "pack",
        (shape_of(BF, 2 * shard, 2 * fs + 2 * fe), shape_of(BF, fs + fe, 2 * shard)), grid=(2,),
        in_specs=[rows_at(fs, theirs), rows_at(fs, theirs), rows_at(fe, theirs), rows_at(fe, theirs),
                  cols_at(fs, theirs), cols_at(fe, theirs)],
        out_specs=(pl.BlockSpec((shard, 2 * fs + 2 * fe), lambda j, s: (j, 0)),
                   pl.BlockSpec((fs + fe, shard), lambda j, s: (0, j))),
    )(here, gs, us, gr, ur, ds, dr)
    in_side = swapped(in_side, "core")
    out_side = swapped(out_side, "core")

    def turned(v):
        return v[:, 0].transpose(0, 2, 1)

    sq = shape_of(BF, tokens, tokens)
    tall = shape_of(BF, tokens, 8 * experts)
    tab = whole((2, expert_ids.shape[3], tokens))
    sel_f, sel_s, sel_c, scale, add_hi, add_lo, add_b = call(
        tables_body, "tables", (sq, sq, sq, shape_of(F32, tokens, 1), tall, tall, tall),
        in_specs=[tab] * 4,
        out_specs=(whole(sq.shape),) * 3 + (whole((tokens, 1)),) + (whole(tall.shape),) * 3,
    )(here, turned(expert_ids), turned(keep_mask), turned(slot_pos), turned(weight_q))

    act = whole((tokens, shard))
    parcel = call(
        parcel_body, "parcel", shape_of(BF, tokens, shard),
        in_specs=[whole(sq.shape)] * 3 + [whole((tokens, 1))] + [act] * 3, out_specs=act,
    )(here, sel_f, sel_s, sel_c, scale, fwd, saved, cot)
    parcel = lax.all_to_all(parcel.reshape(experts, PAD, shard), "y", 0, 0, tiled=True)
    rows = experts * 3 * CAP
    fan = call(
        fan_body, "fan", shape_of(BF, 4, rows, shard),
        in_specs=[act], out_specs=whole((4, rows, shard)),
    )(here, parcel.reshape(tokens, shard))
    got = lax.all_to_all(fan, ("xh", "xl"), 0, 0, tiled=True).reshape(2, 2, rows, shard)

    far_f = swapped(fwd, "xl")
    far_c = swapped(cot, "xl")

    def weight_specs(fw, block, at, mine):
        lane = block * 2
        return [rows_at(fw, mine), rows_at(fw, mine), cols_at(fw, mine),
                pl.BlockSpec((shard, fw), lambda j, s: (at(j, s), lane)),
                pl.BlockSpec((shard, fw), lambda j, s: (at(j, s), lane + 1)),
                pl.BlockSpec((fw, shard), lambda j, s: (lane, at(j, s)))]

    def near_first(j, s):
        return (s[0] + j) % 2

    def far_first(j, s):
        return (s[0] + 1 + j) % 2

    def straight(j, s):
        return j

    def own(at):
        return lambda j, s: 2 * at(j, s) + s[1]

    shared_w = (gs, us, ds, in_side, in_side, out_side)
    routed_w = (gr, ur, dr, in_side, in_side, out_side)

    z_s = call(
        shared_pre_body, "shared_pre", shape_of(F32, 5 * tokens, 2 * fs), grid=(2,),
        in_specs=[act] * 6 + weight_specs(fs, 0, near_first, own(near_first)),
        out_specs=whole((5 * tokens, 2 * fs)),
    )(here, fwd, saved, cot, far_f, far_s, far_c, *shared_w)
    z_s2 = swapped(z_s, "core")

    n_e = 2 * experts * 2 * CAP
    routed_specs = [rows_at(fe, own(straight)), rows_at(fe, own(straight)), cols_at(fe, own(straight)),
                    pl.BlockSpec((shard, fe), lambda j, s: (j, 2 * fs // fe)),
                    pl.BlockSpec((shard, fe), lambda j, s: (j, 2 * fs // fe + 1)),
                    pl.BlockSpec((fe, shard), lambda j, s: (fs // fe, j))]
    z_e = call(
        expert_pre_body, "expert_pre", shape_of(F32, 5 * n_e // 2, 2 * fe), grid=(2,),
        in_specs=[pl.BlockSpec((2, 1, rows, shard), lambda j, s: (0, j, 0, 0))] + routed_specs,
        out_specs=whole((5 * n_e // 2, 2 * fe)),
    )(here, got, *routed_w)
    z_e2 = swapped(z_e, "core")

    ret = call(
        expert_post_body, "expert_post", shape_of(BF, 2, 2, n_e // 2, shard), grid=(2,),
        in_specs=[whole(z_e.shape)] * 2 + routed_specs,
        out_specs=pl.BlockSpec((2, 1, n_e // 2, shard), lambda j, s: (0, j, 0, 0)),
        scratch=[pltpu.VMEM((n_e, 2 * fe), BF)] * 3,
    )(here, z_e, z_e2, *routed_w)
    ret = lax.all_to_all(ret.reshape(4, n_e // 2, shard), ("xh", "xl"), 0, 0, tiled=True)
    ret = jnp.sum(ret.astype(F32), axis=0).astype(BF)
    ret = lax.all_to_all(ret.reshape(experts, 2 * CAP, shard), "y", 0, 0, tiled=True)

    send, keep = call(
        shared_post_body, "shared_post", (shape_of(BF, 2, tokens, shard), shape_of(F32, 2, tokens, shard)), grid=(2,),
        in_specs=[whole(z_s.shape)] * 2 + weight_specs(fs, 0, far_first, own(far_first)),
        out_specs=(whole((2, tokens, shard)), whole((2, tokens, shard))),
        scratch=[pltpu.VMEM((tokens, 2 * fs), BF)] * 3,
    )(here, z_s, z_s2, *shared_w)
    far = swapped(send, "xl")

    out, grad = call(
        merge_body, "merge", (shape_of(BF, tokens, shard),) * 2,
        in_specs=[whole((8 * experts, shard)), whole(keep.shape), whole(far.shape)] + [whole(tall.shape)] * 3,
        out_specs=(act, act),
    )(here, ret.reshape(8 * experts, shard), keep, far, add_hi, add_lo, add_b)
    return out[None], grad[None]


def solution(mesh):
    pipe, expert, tensor = mesh.devices.shape
    fine = Mesh(mesh.devices.reshape(pipe, expert // 2, 2, 2, tensor // 2), ("pipe", "y", "xh", "xl", "core"))
    e, t = ("y", "xh"), ("xl", "core")
    act = P("pipe", e, t)
    table = P(None, "pipe", e, None)
    return jax.shard_map(
        local,
        mesh=fine,
        in_specs=(act, act, act, table, table, table, table,
                  P("pipe", e, None, t), P("pipe", e, None, t), P("pipe", e, t, None),
                  P("pipe", None, t), P("pipe", None, t), P("pipe", t, None)),
        out_specs=(act, act),
        check_vma=False,
    )
```

```python
import jax
import jax.numpy as jnp
from jax import lax
from jax.experimental import pallas as pl
from jax.experimental.pallas import tpu as pltpu
from jax.sharding import Mesh, PartitionSpec as P


BF = jnp.bfloat16
F32 = jnp.float32
I32 = jnp.int32
CAP = 4
PAD = 4 * CAP


def call(body, outs, grid=(1,), in_specs=None, out_specs=None, scratch=(), flops=0):
    spec = pltpu.PrefetchScalarGridSpec(
        num_scalar_prefetch=1, grid=grid, in_specs=in_specs, out_specs=out_specs, scratch_shapes=scratch
    )
    return pl.pallas_call(
        body, grid_spec=spec, out_shape=outs,
        cost_estimate=pl.CostEstimate(flops=flops, transcendentals=0, bytes_accessed=0),
        compiler_params=pltpu.CompilerParams(vmem_limit_bytes=20 * 2**20),
    )


def whole(shape):
    return pl.BlockSpec(shape, lambda j, s: (0,) * len(shape))


hbm = pl.BlockSpec(memory_space=pltpu.HBM)
anywhere = pl.BlockSpec(memory_space=pl.ANY)


def shape_of(dtype, *dims):
    return jax.ShapeDtypeStruct(dims, dtype)


def shifted(block, axis, distance):
    n = lax.axis_size(axis)
    return lax.ppermute(block, axis, [((i - distance) % n, i) for i in range(n)])


def swapped(block, axis):
    return lax.ppermute(block, axis, [(0, 1), (1, 0)])


def dot(a, b):
    return jnp.dot(a, b, preferred_element_type=F32)


def contract_last(left, right):
    return lax.dot_general(left, right, (((1,), (1,)), ((), ())), preferred_element_type=F32)


def tables_body(s, ids, keep, slot, wq, sel_f, sel_s, sel_c, scale):
    tokens = ids.shape[2]
    row = lax.broadcasted_iota(I32, (tokens, 1), 0)
    arr = (row // CAP) % 4
    slot_id = (row // PAD) * CAP + row % CAP
    want_f = jnp.where(arr == 0, slot_id, -1)
    want_b = jnp.where((arr == 1) | (arr == 2), slot_id, -1)
    hit_f = jnp.zeros((tokens, tokens), F32)
    hit_b = jnp.zeros((tokens, tokens), F32)
    weight = jnp.zeros((tokens, tokens), F32)
    target = jnp.where(keep[...] > 0, ids[...] * CAP + slot[...], -2)
    level = wq[1].astype(F32) * (1.0 / 4096.0)
    for k in range(ids.shape[1]):
        hit_f += jnp.where(target[0, k : k + 1] == want_f, 1.0, 0.0)
        eq = target[1, k : k + 1] == want_b
        hit_b += jnp.where(eq, 1.0, 0.0)
        weight += jnp.where(eq, level[k : k + 1], 0.0)
    sel_f[...] = hit_f.astype(BF)
    sel_s[...] = jnp.where(arr == 1, hit_b, 0.0).astype(BF)
    sel_c[...] = jnp.where(arr == 2, hit_b, 0.0).astype(BF)
    scale[...] = jnp.sum(weight, axis=1, keepdims=True)


def adders_body(s, ids, keep, slot, wq, add_hi, add_lo, add_b):
    tokens = ids.shape[2]
    back = add_b.shape[1]
    row = lax.broadcasted_iota(I32, (back, 1), 0)
    dirn = (row // CAP) % 2
    slot_id = (row // 8) * CAP + row % CAP
    back_f = jnp.where(dirn == 0, slot_id, -1)
    back_b = jnp.where(dirn == 1, slot_id, -1)
    hi = jnp.zeros((back, tokens), F32)
    lo = jnp.zeros((back, tokens), F32)
    one = jnp.zeros((back, tokens), F32)
    target = jnp.where(keep[...] > 0, ids[...] * CAP + slot[...], -2)
    level = wq[0]
    top = (level // 64) * 64
    high = top.astype(F32) * (1.0 / 4096.0)
    low = (level - top).astype(F32) * (1.0 / 4096.0)
    for k in range(ids.shape[1]):
        eq = target[0, k : k + 1] == back_f
        hi += jnp.where(eq, high[k : k + 1], 0.0)
        lo += jnp.where(eq, low[k : k + 1], 0.0)
        one += jnp.where(target[1, k : k + 1] == back_b, 1.0, 0.0)
    add_hi[...] = hi.T.astype(BF)
    add_lo[...] = lo.T.astype(BF)
    add_b[...] = one.T.astype(BF)


def parcel_body(s, sel_f, sel_s, sel_c, scale, fwd, saved, cot, out, pair):
    rows = dot(sel_f[...], fwd[...]) + dot(sel_s[...], saved[...]) + scale[...] * dot(sel_c[...], cot[...])
    out[...] = rows.astype(BF)
    pair[0] = fwd[...]
    pair[1] = cot[...]


def fan_body(s, got, out):
    n = got.shape[0]
    m = n * 3 // 4
    half = n // 2
    r = lax.broadcasted_iota(I32, (m, n), 0)
    c = lax.broadcasted_iota(I32, (m, n), 1)
    k = r - half
    source = jnp.where(r < half, (r // 8) * PAD + r % 8, (k // CAP) * PAD + 8 + k % CAP)
    rows = dot(jnp.where(c == source, 1.0, 0.0).astype(BF), got[...]).astype(BF)
    for i in range(out.shape[0]):
        out[i] = rows


def run(copies, sems):
    handles = [pltpu.make_async_copy(src, dst, sems.at[i]) for i, (src, dst) in enumerate(copies)]
    for h in handles:
        h.start()

    def wait(lo, hi):
        for h in handles[lo:hi]:
            h.wait()

    return wait


def pack_body(s, gs, us, gr, ur, ds, dr, box, hold, sems):
    w = gs.shape[2]
    n = gr.shape[2]
    f = gs.shape[1]
    wait = []
    for x in range(2):
        t = 2 * x + 1 - s[1]
        cols = pl.ds(pl.multiple_of(t * f, 128), f)
        h = hold.at[x]
        wait.append(run([
            (gs.at[t], h.at[0:f, 0:w]),
            (us.at[t], h.at[0:f, w : 2 * w]),
            (gr.at[t], h.at[0:f, 2 * w : 2 * w + n]),
            (ur.at[t], h.at[0:f, 2 * w + n : 2 * w + 2 * n]),
            (dr.at[:, cols], h.at[f : f + n]),
            (ds.at[:, cols], h.at[f + n :]),
        ], sems.at[7 * x :]))
    done = []
    for x in range(2):
        wait[x](0, 6)
        done.append(run([(hold.at[x], box.at[x])], sems.at[7 * x + 6 :]))
    for x in range(2):
        done[x](0, 1)


def weight_copies(s, order, gate, up, down, box, lane, row, g, u, d):
    f, w = gate.shape[1:]
    gates, ups, downs = [], [], []
    for i, x in enumerate(order):
        t = 2 * x + s[1]
        rows = slice(i * f, i * f + f)
        body = box.at[x, 0:f]
        gates += [(gate.at[t], g.at[rows, 0:w]), (body.at[:, lane : lane + w], g.at[rows, w : 2 * w])]
        ups += [(up.at[t], u.at[rows, 0:w]), (body.at[:, lane + w : lane + 2 * w], u.at[rows, w : 2 * w])]
        downs += [(down.at[:, pl.ds(pl.multiple_of(t * f, 128), f)], d.at[0:w, rows]),
                  (box.at[x, row : row + w], d.at[w : 2 * w, rows])]
    return gates, ups, downs


def joined(mine, other):
    w = mine.shape[1] // 2
    return jnp.concatenate([mine[:, :w] + other[:, w:], mine[:, w:] + other[:, :w]], axis=1)


def pre(wait, n_x, both, cot, g, u, d, acc):
    n = both.shape[0]
    wait(0, n_x + 4)
    acc[0:n] = dot(both[...], g[...])
    wait(n_x + 4, n_x + 8)
    acc[n : 2 * n] = dot(both[...], u[...])
    wait(n_x + 8, n_x + 12)
    acc[2 * n :] = contract_last(cot[...], d[...])


def shared_pre_body(s, fwd, saved, cot, far, far_s, gate, up, down, box, acc, x, g, u, d, sems):
    n, f = fwd.shape
    near, away = slice(0, f), slice(f, 2 * f)
    xs = [(fwd, x.at[0:n, near]), (saved, x.at[n : 2 * n, near]), (cot, x.at[2 * n :, near]),
          (far.at[0], x.at[0:n, away]), (far_s, x.at[n : 2 * n, away]), (far.at[1], x.at[2 * n :, away])]
    ws = weight_copies(s, (s[0], 1 - s[0]), gate, up, down, box, 0, f + gate.shape[2] // 2, g, u, d)
    wait = run(xs + ws[0] + ws[1] + ws[2], sems)
    pre(wait, len(xs), x.at[0 : 2 * n], x.at[2 * n :], g, u, d, acc)


def shared_post_body(s, mine, other, gate, up, down, gate_o, up_o, down_o, send, keep, hid, gg, gu):
    j = pl.program_id(0)
    n = hid.shape[0]
    w = gate.shape[2]

    @pl.when(j == 0)
    def _():
        a_f = joined(mine[0:n], other[0:n])
        a_s = joined(mine[n : 2 * n], other[n : 2 * n])
        b_f = joined(mine[2 * n : 3 * n], other[2 * n : 3 * n])
        b_s = joined(mine[3 * n : 4 * n], other[3 * n : 4 * n])
        dh = joined(mine[4 * n : 5 * n], other[4 * n : 5 * n])
        hid[...] = (a_f * jax.nn.sigmoid(a_f) * b_f).astype(BF)
        sg = jax.nn.sigmoid(a_s)
        gg[...] = (dh * b_s * (sg * (1.0 + a_s * (1.0 - sg)))).astype(BF)
        gu[...] = (dh * (a_s * sg)).astype(BF)

    out = dot(hid[:, :w], down[...]) + dot(hid[:, w:], down_o[0])
    grad = (
        contract_last(gg[:, :w], gate[0]) + contract_last(gg[:, w:], gate_o[0])
        + contract_last(gu[:, :w], up[0]) + contract_last(gu[:, w:], up_o[0])
    )

    @pl.when(j == 0)
    def _():
        send[0] = out.astype(BF)
        send[1] = grad.astype(BF)

    @pl.when(j == 1)
    def _():
        keep[0] = out
        keep[1] = grad


def expert_pre_body(s, got, gate, up, down, box, acc, both, cot, g, u, d, sems):
    n, f = both.shape[0] // 2, got.shape[3]
    m = cot.shape[0] // 2
    xs = []
    for h in range(2):
        for x in range(2):
            cols = slice(x * f, x * f + f)
            xs += [(got.at[h, x, 0:n], both.at[h * n : h * n + n, cols]),
                   (got.at[h, x, n:], cot.at[h * m : h * m + m, cols])]
    w = gate.shape[2]
    ws = weight_copies(s, (0, 1), gate, up, down, box, 4 * w, f, g, u, d)
    wait = run(xs + ws[0] + ws[1] + ws[2], sems)
    pre(wait, len(xs), both, cot, g, u, d, acc)


def expert_post_body(s, mine, other, gate, up, down, gate_o, up_o, down_o, out, hid, gg, gu):
    j = pl.program_id(0)
    n = hid.shape[0]
    m = n // 2
    w = gate.shape[2]

    @pl.when(j == 0)
    def _():
        a = joined(mine[0:n], other[0:n])
        b = joined(mine[n : 2 * n], other[n : 2 * n])
        dh = joined(mine[2 * n : 2 * n + m], other[2 * n : 2 * n + m])
        r = lax.broadcasted_iota(I32, (n, m), 0)
        c = lax.broadcasted_iota(I32, (n, m), 1)
        place = jnp.where(c == (r // 8) * CAP + r % CAP, 1.0, 0.0)
        dh = jnp.dot(place, dh, precision=lax.Precision.HIGHEST, preferred_element_type=F32)
        back = (lax.broadcasted_iota(I32, (n, 1), 0) // CAP) % 2 == 1
        sg = jax.nn.sigmoid(a)
        hid[...] = jnp.where(back, 0.0, a * sg * b).astype(BF)
        gg[...] = jnp.where(back, dh * b * (sg * (1.0 + a * (1.0 - sg))), 0.0).astype(BF)
        gu[...] = jnp.where(back, dh * (a * sg), 0.0).astype(BF)

    rows = (
        dot(hid[:, :w], down[...]) + dot(hid[:, w:], down_o[0])
        + contract_last(gg[:, :w], gate[0]) + contract_last(gg[:, w:], gate_o[0])
        + contract_last(gu[:, :w], up[0]) + contract_last(gu[:, w:], up_o[0])
    ).astype(BF)
    out[0, 0] = rows[:m]
    out[1, 0] = rows[m:]


def sum_body(s, parts, out):
    p = parts[...].astype(F32)
    out[...] = ((p[0] + p[1]) + (p[2] + p[3])).astype(BF)


def merge_body(s, back, keep, far, add_hi, add_lo, add_b, out, grad):
    rows = back[...]
    out[...] = (keep[0] + far[0].astype(F32) + (dot(add_hi[...], rows) + dot(add_lo[...], rows))).astype(BF)
    grad[...] = (keep[1] + far[1].astype(F32) + dot(add_b[...], rows)).astype(BF)


def local(inputs_prev, cotangent_next, saved_input, expert_ids, keep_mask, slot_pos, weight_q,
          gate_routed, up_routed, down_routed, gate_shared, up_shared, down_shared):
    tokens, shard = inputs_prev.shape[1:]
    experts = lax.axis_size("y")
    here = jnp.stack([lax.axis_index("xl"), lax.axis_index("core")]).astype(I32)
    saved = saved_input[0]
    gs = gate_shared[0].reshape(4, shard, -1)
    us = up_shared[0].reshape(4, shard, -1)
    ds = down_shared[0]
    gr = gate_routed[0, 0].reshape(4, shard, -1)
    ur = up_routed[0, 0].reshape(4, shard, -1)
    dr = down_routed[0, 0]
    gs, us, ds, gr, ur, dr = [pltpu.with_memory_space_constraint(w, pltpu.HBM) for w in (gs, us, ds, gr, ur, dr)]
    fs = gs.shape[2]
    fe = gr.shape[2]

    fwd = shifted(inputs_prev[0], "pipe", 1)
    cot = shifted(cotangent_next[0], "pipe", -1)
    far_s = swapped(saved, "xl")

    def rows_at(n, which):
        return pl.BlockSpec((1, shard, n), lambda j, s: (which(j, s), 0, 0))

    def cols_at(n, which):
        return pl.BlockSpec((n, shard), lambda j, s: (0, which(j, s)))

    height = shard + fe + fs
    box = call(
        pack_body, pltpu.HBM((2, height, shard), BF), in_specs=[hbm] * 6, out_specs=hbm,
        scratch=[pltpu.VMEM((2, height, shard), BF), pltpu.SemaphoreType.DMA((14,))],
    )(here, gs, us, gr, ur, ds, dr)
    box = swapped(box, "core")

    def turned(v):
        return pltpu.with_memory_space_constraint(v[:, 0].transpose(0, 2, 1), pltpu.HBM)

    sq = shape_of(BF, tokens, tokens)
    tall = shape_of(BF, tokens, 8 * experts)
    tab = whole((2, expert_ids.shape[3], tokens))
    plan = [turned(v) for v in (expert_ids, keep_mask, slot_pos, weight_q)]
    sel_f, sel_s, sel_c, scale = call(
        tables_body, (sq, sq, sq, shape_of(F32, tokens, 1)),
        in_specs=[tab] * 4, out_specs=(whole(sq.shape),) * 3 + (whole((tokens, 1)),),
    )(here, *plan)
    add_hi, add_lo, add_b = call(
        adders_body, (tall, tall, tall), in_specs=[tab] * 4, out_specs=(whole(tall.shape),) * 3,
    )(here, *plan)

    act = whole((tokens, shard))
    parcel, pair = call(
        parcel_body, (pltpu.HBM((tokens, shard), BF), pltpu.HBM((2, tokens, shard), BF)),
        in_specs=[whole(sq.shape)] * 3 + [whole((tokens, 1))] + [act] * 3, out_specs=(act, whole((2, tokens, shard))),
    )(here, sel_f, sel_s, sel_c, scale, fwd, saved, cot)
    parcel = lax.all_to_all(parcel.reshape(experts, PAD, shard), "y", 0, 0, tiled=True)
    rows = experts * 3 * CAP
    fan = call(
        fan_body, pltpu.HBM((4, rows, shard), BF),
        in_specs=[act], out_specs=whole((4, rows, shard)),
    )(here, parcel.reshape(tokens, shard))
    got = lax.all_to_all(fan, ("xh", "xl"), 0, 0, tiled=True).reshape(2, 2, rows, shard)

    far_fc = swapped(pair, "xl")

    def buffers(w):
        return [pltpu.VMEM((2 * shard, 2 * w), BF)] * 2 + [pltpu.VMEM((2 * w, 2 * shard), BF)]

    def weight_specs(w, lane, row, at):
        mine = lambda j, s: 2 * at(j, s) + s[1]
        return [rows_at(w, mine), rows_at(w, mine), cols_at(w, mine),
                pl.BlockSpec((1, shard, w), lambda j, s: (at(j, s), 0, lane)),
                pl.BlockSpec((1, shard, w), lambda j, s: (at(j, s), 0, lane + 1)),
                pl.BlockSpec((1, w, shard), lambda j, s: (at(j, s), row, 0))]

    far_first = lambda j, s: (s[0] + 1 + j) % 2
    straight = lambda j, s: j

    def sems(n):
        return [pltpu.SemaphoreType.DMA((n,))]

    shared_w = (gs, us, ds, box)
    shared_w2 = (gs, us, ds, box, box, box)
    routed_w = (gr, ur, dr, box)
    routed_w2 = (gr, ur, dr, box, box, box)
    z_shape = (5 * tokens, 2 * fs)
    z_s = call(
        shared_pre_body, shape_of(F32, *z_shape),
        in_specs=[anywhere] * 5 + [hbm] * 3 + [anywhere], out_specs=whole(z_shape),
        scratch=[pltpu.VMEM((3 * tokens, 2 * shard), BF)] + buffers(fs) + sems(18),
    )(here, fwd, saved, cot, far_fc, far_s, *shared_w)
    z_s2 = swapped(z_s, "core")

    n_e = 2 * experts * 2 * CAP
    ze_shape = (5 * n_e // 2, 2 * fe)
    z_e = call(
        expert_pre_body, shape_of(F32, *ze_shape),
        in_specs=[anywhere] + [hbm] * 3 + [anywhere], out_specs=whole(ze_shape),
        scratch=[pltpu.VMEM((n_e, 2 * shard), BF), pltpu.VMEM((n_e // 2, 2 * shard), BF)] + buffers(fe) + sems(20),
    )(here, got, *routed_w)
    z_e2 = swapped(z_e, "core")

    ret = call(
        expert_post_body, pltpu.HBM((2, 2, n_e // 2, shard), BF), grid=(2,),
        in_specs=[whole(ze_shape)] * 2 + weight_specs(fe, 2 * fs // fe, shard // fe, straight),
        out_specs=pl.BlockSpec((2, 1, n_e // 2, shard), lambda j, s: (0, j, 0, 0)),
        scratch=[pltpu.VMEM((n_e, 2 * fe), BF)] * 3,
    )(here, z_e, z_e2, *routed_w2)
    ret = lax.all_to_all(ret.reshape(4, n_e // 2, shard), ("xh", "xl"), 0, 0, tiled=True)
    ret = call(
        sum_body, pltpu.HBM((n_e // 2, shard), BF),
        in_specs=[whole((4, n_e // 2, shard))], out_specs=whole((n_e // 2, shard)),
    )(here, ret)
    ret = lax.all_to_all(ret.reshape(experts, 2 * CAP, shard), "y", 0, 0, tiled=True)

    send, keep = call(
        shared_post_body, (pltpu.HBM((2, tokens, shard), BF), pltpu.HBM((2, tokens, shard), F32)), grid=(2,),
        in_specs=[whole(z_shape)] * 2 + weight_specs(fs, 0, (shard + fe) // fs, far_first),
        out_specs=(whole((2, tokens, shard)),) * 2,
        scratch=[pltpu.VMEM((tokens, 2 * fs), BF)] * 3,
    )(here, z_s, z_s2, *shared_w2)
    far = swapped(send, "xl")

    keep = pltpu.with_memory_space_constraint(keep, pltpu.HBM)
    out, grad = call(
        merge_body, (shape_of(BF, tokens, shard),) * 2,
        in_specs=[whole((8 * experts, shard)), whole(keep.shape), whole(far.shape)] + [whole(tall.shape)] * 3,
        out_specs=(act, act),
    )(here, ret.reshape(8 * experts, shard), keep, far, add_hi, add_lo, add_b)
    return out[None], grad[None]


def solution(mesh):
    pipe, expert, tensor = mesh.devices.shape
    fine = Mesh(mesh.devices.reshape(pipe, expert // 2, 2, 2, tensor // 2), ("pipe", "y", "xh", "xl", "core"))
    e, t = ("y", "xh"), ("xl", "core")
    act = P("pipe", e, t)
    table = P(None, "pipe", e, None)

    def step(*args):
        return local(*args)

    step = jax.shard_map(
        step,
        mesh=fine,
        in_specs=(act, act, act, table, table, table, table,
                  P("pipe", e, None, t), P("pipe", e, None, t), P("pipe", e, t, None),
                  P("pipe", None, t), P("pipe", None, t), P("pipe", t, None)),
        out_specs=(act, act),
        check_vma=False,
    )


    return step
```

```python
import jax
import jax.numpy as jnp
from jax import lax
from jax.experimental import pallas as pl
from jax.experimental.pallas import tpu as pltpu
from jax.sharding import Mesh, PartitionSpec as P


BF = jnp.bfloat16
F32 = jnp.float32
I32 = jnp.int32
CAP = 4
PAD = 4 * CAP


def call(body, outs, grid=(1,), in_specs=None, out_specs=None, scratch=(), flops=0, aliases={}):
    spec = pltpu.PrefetchScalarGridSpec(
        num_scalar_prefetch=1, grid=grid, in_specs=in_specs, out_specs=out_specs, scratch_shapes=scratch
    )
    return pl.pallas_call(
        body, grid_spec=spec, out_shape=outs, input_output_aliases=aliases,
        cost_estimate=pl.CostEstimate(flops=flops, transcendentals=0, bytes_accessed=0),
        compiler_params=pltpu.CompilerParams(vmem_limit_bytes=20 * 2**20),
    )


def whole(shape):
    return pl.BlockSpec(shape, lambda j, s: (0,) * len(shape))


hbm = pl.BlockSpec(memory_space=pltpu.HBM)
anywhere = pl.BlockSpec(memory_space=pl.ANY)


def shape_of(dtype, *dims):
    return jax.ShapeDtypeStruct(dims, dtype)


def shifted(block, axis, distance):
    n = lax.axis_size(axis)
    return lax.ppermute(block, axis, [((i - distance) % n, i) for i in range(n)])


def swapped(block, axis):
    return lax.ppermute(block, axis, [(0, 1), (1, 0)])


def dot(a, b):
    return jnp.dot(a, b, preferred_element_type=F32)


def contract_last(left, right):
    return lax.dot_general(left, right, (((1,), (1,)), ((), ())), preferred_element_type=F32)


def make_tables(ids, keep, slot, wq, sel, scale):
    tokens = ids.shape[2]
    row = lax.broadcasted_iota(I32, (tokens, 1), 0)
    arr = (row // CAP) % 4
    slot_id = (row // PAD) * CAP + row % CAP
    want_f = jnp.where(arr == 0, slot_id, -1)
    want_b = jnp.where((arr == 1) | (arr == 2), slot_id, -1)
    hit_f = jnp.zeros((tokens, tokens), F32)
    hit_b = jnp.zeros((tokens, tokens), F32)
    weight = jnp.zeros((tokens, tokens), F32)
    target = jnp.where(keep[...] > 0, ids[...] * CAP + slot[...], -2)
    level = wq[1].astype(F32) * (1.0 / 4096.0)
    for k in range(ids.shape[1]):
        hit_f += jnp.where(target[0, k : k + 1] == want_f, 1.0, 0.0)
        eq = target[1, k : k + 1] == want_b
        hit_b += jnp.where(eq, 1.0, 0.0)
        weight += jnp.where(eq, level[k : k + 1], 0.0)
    sel[0] = hit_f.astype(BF)
    sel[1] = jnp.where(arr == 1, hit_b, 0.0).astype(BF)
    sel[2] = jnp.where(arr == 2, hit_b, 0.0).astype(BF)
    scale[...] = jnp.broadcast_to(jnp.sum(weight, axis=1, keepdims=True), scale.shape)


def adders_body(s, ids, keep, slot, wq, add_hi, add_lo, add_b):
    tokens = ids.shape[2]
    back = add_b.shape[1]
    row = lax.broadcasted_iota(I32, (back, 1), 0)
    dirn = (row // CAP) % 2
    slot_id = (row // 8) * CAP + row % CAP
    back_f = jnp.where(dirn == 0, slot_id, -1)
    back_b = jnp.where(dirn == 1, slot_id, -1)
    hi = jnp.zeros((back, tokens), F32)
    lo = jnp.zeros((back, tokens), F32)
    one = jnp.zeros((back, tokens), F32)
    target = jnp.where(keep[...] > 0, ids[...] * CAP + slot[...], -2)
    level = wq[0]
    top = (level // 64) * 64
    high = top.astype(F32) * (1.0 / 4096.0)
    low = (level - top).astype(F32) * (1.0 / 4096.0)
    for k in range(ids.shape[1]):
        eq = target[0, k : k + 1] == back_f
        hi += jnp.where(eq, high[k : k + 1], 0.0)
        lo += jnp.where(eq, low[k : k + 1], 0.0)
        one += jnp.where(target[1, k : k + 1] == back_b, 1.0, 0.0)
    add_hi[...] = hi.T.astype(BF)
    add_lo[...] = lo.T.astype(BF)
    add_b[...] = one.T.astype(BF)


def parcel_body(s, sel, scale, fwd, saved, cot, out, pair):
    rows = dot(sel[0], fwd[...]) + dot(sel[1], saved[...]) + scale[:, 0:1] * dot(sel[2], cot[...])
    out[...] = rows.astype(BF)
    pair[0] = fwd[...]
    pair[1] = cot[...]


def fan_body(s, got, out):
    n = got.shape[0]
    m = n * 3 // 4
    half = n // 2
    r = lax.broadcasted_iota(I32, (m, n), 0)
    c = lax.broadcasted_iota(I32, (m, n), 1)
    k = r - half
    source = jnp.where(r < half, (r // 8) * PAD + r % 8, (k // CAP) * PAD + 8 + k % CAP)
    rows = dot(jnp.where(c == source, 1.0, 0.0).astype(BF), got[...]).astype(BF)
    for i in range(out.shape[0]):
        out[i] = rows


def run(copies, sems):
    handles = [pltpu.make_async_copy(src, dst, sems.at[i]) for i, (src, dst) in enumerate(copies)]
    for h in handles:
        h.start()

    def wait(lo, hi):
        for h in handles[lo:hi]:
            h.wait()

    return wait


def prep(gs, us, gr, ur, ds, dr, plan, box, sel, scale, hold, ints, sel_v, scale_v, sems, s):
    w = gs.shape[2]
    n = gr.shape[2]
    f = gs.shape[1]
    ready = run([(v, ints.at[i]) for i, v in enumerate(plan)], sems.at[14:18])
    wait = []
    for x in range(2):
        t = 2 * x + 1 - s[1]
        cols = pl.ds(pl.multiple_of(t * f, 128), f)
        h = hold.at[x]
        wait.append(run([
            (gs.at[t], h.at[0:f, 0:w]),
            (us.at[t], h.at[0:f, w : 2 * w]),
            (gr.at[t], h.at[0:f, 2 * w : 2 * w + n]),
            (ur.at[t], h.at[0:f, 2 * w + n : 2 * w + 2 * n]),
            (dr.at[:, cols], h.at[f : f + n]),
            (ds.at[:, cols], h.at[f + n :]),
        ], sems.at[7 * x : 7 * x + 6]))
    ready(0, 4)
    make_tables(*[ints.at[i] for i in range(4)], sel_v, scale_v)
    done = [run([(sel_v, sel), (scale_v, scale)], sems.at[18:20])]
    for x in range(2):
        wait[x](0, 6)
        done.append(run([(hold.at[x], box.at[x])], sems.at[7 * x + 6 : 7 * x + 7]))
    done[0](0, 2)
    done[1](0, 1)
    done[2](0, 1)


def prep_first_body(s, *refs):
    @pl.when(s[2] == 0)
    def _():
        prep(*refs[:6], refs[6:10], *refs[10:], s)


def prep_rest_body(s, *refs):
    @pl.when(s[2] != 0)
    def _():
        prep(*refs[:6], refs[6:10], *refs[13:], s)


def weight_copies(s, order, gate, up, down, box, lane, row, g, u, d):
    f, w = gate.shape[1:]
    gates, ups, downs = [], [], []
    for i, x in enumerate(order):
        t = 2 * x + s[1]
        rows = slice(i * f, i * f + f)
        body = box.at[x, 0:f]
        gates += [(gate.at[t], g.at[rows, 0:w]), (body.at[:, lane : lane + w], g.at[rows, w : 2 * w])]
        ups += [(up.at[t], u.at[rows, 0:w]), (body.at[:, lane + w : lane + 2 * w], u.at[rows, w : 2 * w])]
        downs += [(down.at[:, pl.ds(pl.multiple_of(t * f, 128), f)], d.at[0:w, rows]),
                  (box.at[x, row : row + w], d.at[w : 2 * w, rows])]
    return gates, ups, downs


def joined(mine, other):
    w = mine.shape[1] // 2
    return jnp.concatenate([mine[:, :w] + other[:, w:], mine[:, w:] + other[:, :w]], axis=1)


def pre(wait, n_x, both, cot, g, u, d, acc):
    n = both.shape[0]
    wait(0, n_x + 4)
    acc[0:n] = dot(both[...], g[...])
    wait(n_x + 4, n_x + 8)
    acc[n : 2 * n] = dot(both[...], u[...])
    wait(n_x + 8, n_x + 12)
    acc[2 * n :] = contract_last(cot[...], d[...])


def shared_pre_body(s, fwd, saved, cot, far, far_s, gate, up, down, box, acc, x, g, u, d, sems):
    n, f = fwd.shape
    near, away = slice(0, f), slice(f, 2 * f)
    xs = [(fwd, x.at[0:n, near]), (saved, x.at[n : 2 * n, near]), (cot, x.at[2 * n :, near]),
          (far.at[0], x.at[0:n, away]), (far_s, x.at[n : 2 * n, away]), (far.at[1], x.at[2 * n :, away])]
    ws = weight_copies(s, (s[0], 1 - s[0]), gate, up, down, box, 0, f + gate.shape[2] // 2, g, u, d)
    wait = run(xs + ws[0] + ws[1] + ws[2], sems)
    pre(wait, len(xs), x.at[0 : 2 * n], x.at[2 * n :], g, u, d, acc)


def shared_back(hid, gg, gu, gate, up, down, gate_o, up_o, down_o):
    w = gate.shape[2]
    out = dot(hid[:, :w], down[...]) + dot(hid[:, w:], down_o[0])
    grad = (
        contract_last(gg[:, :w], gate[0]) + contract_last(gg[:, w:], gate_o[0])
        + contract_last(gu[:, :w], up[0]) + contract_last(gu[:, w:], up_o[0])
    )
    return out, grad


def shared_send_body(s, mine, other, gate, up, down, gate_o, up_o, down_o, send, hid_out, gg_out, gu_out):
    n = send.shape[1]
    a_f, a_s, b_f, b_s, dh = [joined(mine[i * n : i * n + n], other[i * n : i * n + n]) for i in range(5)]
    hid = (a_f * jax.nn.sigmoid(a_f) * b_f).astype(BF)
    sg = jax.nn.sigmoid(a_s)
    gg = (dh * b_s * (sg * (1.0 + a_s * (1.0 - sg)))).astype(BF)
    gu = (dh * (a_s * sg)).astype(BF)
    hid_out[...] = hid
    gg_out[...] = gg
    gu_out[...] = gu
    out, grad = shared_back(hid, gg, gu, gate, up, down, gate_o, up_o, down_o)
    send[0] = out.astype(BF)
    send[1] = grad.astype(BF)


def shared_keep_body(s, hid, gg, gu, gate, up, down, gate_o, up_o, down_o, keep):
    keep[0], keep[1] = shared_back(hid[...], gg[...], gu[...], gate, up, down, gate_o, up_o, down_o)


def expert_pre_body(s, got, gate, up, down, box, acc, both, cot, g, u, d, sems):
    n, f = both.shape[0] // 2, got.shape[3]
    m = cot.shape[0] // 2
    xs = []
    for h in range(2):
        for x in range(2):
            cols = slice(x * f, x * f + f)
            xs += [(got.at[h, x, 0:n], both.at[h * n : h * n + n, cols]),
                   (got.at[h, x, n:], cot.at[h * m : h * m + m, cols])]
    w = gate.shape[2]
    ws = weight_copies(s, (0, 1), gate, up, down, box, 4 * w, f, g, u, d)
    wait = run(xs + ws[0] + ws[1] + ws[2], sems)
    pre(wait, len(xs), both, cot, g, u, d, acc)


def expert_post_body(s, mine, other, gate, up, down, gate_o, up_o, down_o, out, hid, gg, gu):
    j = pl.program_id(0)
    n = hid.shape[0]
    m = n // 2
    w = gate.shape[2]

    @pl.when(j == 0)
    def _():
        a = joined(mine[0:n], other[0:n])
        b = joined(mine[n : 2 * n], other[n : 2 * n])
        dh = joined(mine[2 * n : 2 * n + m], other[2 * n : 2 * n + m])
        r = lax.broadcasted_iota(I32, (n, m), 0)
        c = lax.broadcasted_iota(I32, (n, m), 1)
        place = jnp.where(c == (r // 8) * CAP + r % CAP, 1.0, 0.0)
        dh = jnp.dot(place, dh, precision=lax.Precision.HIGHEST, preferred_element_type=F32)
        back = (lax.broadcasted_iota(I32, (n, 1), 0) // CAP) % 2 == 1
        sg = jax.nn.sigmoid(a)
        hid[...] = jnp.where(back, 0.0, a * sg * b).astype(BF)
        gg[...] = jnp.where(back, dh * b * (sg * (1.0 + a * (1.0 - sg))), 0.0).astype(BF)
        gu[...] = jnp.where(back, dh * (a * sg), 0.0).astype(BF)

    rows = (
        dot(hid[:, :w], down[...]) + dot(hid[:, w:], down_o[0])
        + contract_last(gg[:, :w], gate[0]) + contract_last(gg[:, w:], gate_o[0])
        + contract_last(gu[:, :w], up[0]) + contract_last(gu[:, w:], up_o[0])
    ).astype(BF)
    out[0, 0] = rows[:m]
    out[1, 0] = rows[m:]


def sum_body(s, parts, out):
    p = parts[...].astype(F32)
    out[...] = ((p[0] + p[1]) + (p[2] + p[3])).astype(BF)


def merge_body(s, back, keep, far, add_hi, add_lo, add_b, out, grad):
    rows = back[...]
    out[...] = (keep[0] + far[0].astype(F32) + (dot(add_hi[...], rows) + dot(add_lo[...], rows))).astype(BF)
    grad[...] = (keep[1] + far[1].astype(F32) + dot(add_b[...], rows)).astype(BF)


def local(inputs_prev, cotangent_next, saved_input, expert_ids, keep_mask, slot_pos, weight_q,
          gate_routed, up_routed, down_routed, gate_shared, up_shared, down_shared):
    tokens, shard = inputs_prev.shape[1:]
    experts = lax.axis_size("y")
    here = jnp.stack([lax.axis_index("xl"), lax.axis_index("core"), lax.axis_index("pipe")]).astype(I32)
    saved = saved_input[0]
    gs = gate_shared[0].reshape(4, shard, -1)
    us = up_shared[0].reshape(4, shard, -1)
    ds = down_shared[0]
    gr = gate_routed[0, 0].reshape(4, shard, -1)
    ur = up_routed[0, 0].reshape(4, shard, -1)
    dr = down_routed[0, 0]
    gs, us, ds, gr, ur, dr = [pltpu.with_memory_space_constraint(w, pltpu.HBM) for w in (gs, us, ds, gr, ur, dr)]
    fs = gs.shape[2]
    fe = gr.shape[2]

    fwd = shifted(inputs_prev[0], "pipe", 1)
    cot = shifted(cotangent_next[0], "pipe", -1)
    far_s = swapped(saved, "xl")

    def rows_at(n, which):
        return pl.BlockSpec((1, shard, n), lambda j, s: (which(j, s), 0, 0))

    def cols_at(n, which):
        return pl.BlockSpec((n, shard), lambda j, s: (0, which(j, s)))

    height = shard + fe + fs

    def turned(v):
        return pltpu.with_memory_space_constraint(v[:, 0].transpose(0, 2, 1), pltpu.HBM)

    plan = [turned(v) for v in (expert_ids, keep_mask, slot_pos, weight_q)]
    sq = (tokens, tokens)
    tall = shape_of(BF, tokens, 8 * experts)
    tab = whole((2, expert_ids.shape[3], tokens))
    made = (pltpu.HBM((2, height, shard), BF), pltpu.HBM((3, *sq), BF), pltpu.HBM(sq, F32))
    room = [pltpu.VMEM((2, height, shard), BF), pltpu.VMEM((4, 2, expert_ids.shape[3], tokens), I32),
            pltpu.VMEM((3, *sq), BF), pltpu.VMEM(sq, F32), pltpu.SemaphoreType.DMA((20,))]
    given = (gs, us, gr, ur, ds, dr, *plan)
    first = call(prep_first_body, made, in_specs=[hbm] * 10, out_specs=(hbm,) * 3, scratch=room)(here, *given)
    box, sel, scale = call(
        prep_rest_body, made, in_specs=[hbm] * 13, out_specs=(hbm,) * 3, scratch=room,
        aliases={11: 0, 12: 1, 13: 2},
    )(here, *given, *first)
    box = swapped(box, "core")

    add_hi, add_lo, add_b = call(
        adders_body, (tall, tall, tall), in_specs=[tab] * 4, out_specs=(whole(tall.shape),) * 3,
    )(here, *plan)

    act = whole((tokens, shard))
    parcel, pair = call(
        parcel_body, (pltpu.HBM((tokens, shard), BF), pltpu.HBM((2, tokens, shard), BF)),
        in_specs=[whole((3, *sq)), whole(sq)] + [act] * 3, out_specs=(act, whole((2, tokens, shard))),
    )(here, sel, scale, fwd, saved, cot)
    parcel = lax.all_to_all(parcel.reshape(experts, PAD, shard), "y", 0, 0, tiled=True)
    rows = experts * 3 * CAP
    fan = call(
        fan_body, pltpu.HBM((4, rows, shard), BF),
        in_specs=[act], out_specs=whole((4, rows, shard)),
    )(here, parcel.reshape(tokens, shard))
    got = lax.all_to_all(fan, ("xh", "xl"), 0, 0, tiled=True).reshape(2, 2, rows, shard)

    far_fc = swapped(pair, "xl")

    def buffers(w):
        return [pltpu.VMEM((2 * shard, 2 * w), BF)] * 2 + [pltpu.VMEM((2 * w, 2 * shard), BF)]

    def weight_specs(w, lane, row, at):
        mine = lambda j, s: 2 * at(j, s) + s[1]
        return [rows_at(w, mine), rows_at(w, mine), cols_at(w, mine),
                pl.BlockSpec((1, shard, w), lambda j, s: (at(j, s), 0, lane)),
                pl.BlockSpec((1, shard, w), lambda j, s: (at(j, s), 0, lane + 1)),
                pl.BlockSpec((1, w, shard), lambda j, s: (at(j, s), row, 0))]

    straight = lambda j, s: j

    def sems(n):
        return [pltpu.SemaphoreType.DMA((n,))]

    shared_w = (gs, us, ds, box)
    shared_w2 = (gs, us, ds, box, box, box)
    routed_w = (gr, ur, dr, box)
    routed_w2 = (gr, ur, dr, box, box, box)
    z_shape = (5 * tokens, 2 * fs)
    z_s = call(
        shared_pre_body, shape_of(F32, *z_shape),
        in_specs=[anywhere] * 5 + [hbm] * 3 + [anywhere], out_specs=whole(z_shape),
        scratch=[pltpu.VMEM((3 * tokens, 2 * shard), BF)] + buffers(fs) + sems(18),
    )(here, fwd, saved, cot, far_fc, far_s, *shared_w)
    z_s2 = swapped(z_s, "core")

    n_e = 2 * experts * 2 * CAP
    ze_shape = (5 * n_e // 2, 2 * fe)
    z_e = call(
        expert_pre_body, shape_of(F32, *ze_shape),
        in_specs=[anywhere] + [hbm] * 3 + [anywhere], out_specs=whole(ze_shape),
        scratch=[pltpu.VMEM((n_e, 2 * shard), BF), pltpu.VMEM((n_e // 2, 2 * shard), BF)] + buffers(fe) + sems(20),
    )(here, got, *routed_w)
    z_e2 = swapped(z_e, "core")

    ret = call(
        expert_post_body, pltpu.HBM((2, 2, n_e // 2, shard), BF), grid=(2,),
        in_specs=[whole(ze_shape)] * 2 + weight_specs(fe, 2 * fs // fe, shard // fe, straight),
        out_specs=pl.BlockSpec((2, 1, n_e // 2, shard), lambda j, s: (0, j, 0, 0)),
        scratch=[pltpu.VMEM((n_e, 2 * fe), BF)] * 3,
    )(here, z_e, z_e2, *routed_w2)
    ret = lax.all_to_all(ret.reshape(4, n_e // 2, shard), ("xh", "xl"), 0, 0, tiled=True)
    ret = call(
        sum_body, pltpu.HBM((n_e // 2, shard), BF),
        in_specs=[whole((4, n_e // 2, shard))], out_specs=whole((n_e // 2, shard)),
    )(here, ret)
    ret = lax.all_to_all(ret.reshape(experts, 2 * CAP, shard), "y", 0, 0, tiled=True)

    hid_shape = (tokens, 2 * fs)
    row0 = (shard + fe) // fs
    send, *hidden = call(
        shared_send_body, (pltpu.HBM((2, tokens, shard), BF),) + (pltpu.HBM(hid_shape, BF),) * 3,
        in_specs=[whole(z_shape)] * 2 + weight_specs(fs, 0, row0, lambda j, s: 1 - s[0]),
        out_specs=(whole((2, tokens, shard)),) + (whole(hid_shape),) * 3,
    )(here, z_s, z_s2, *shared_w2)
    hidden = [pltpu.with_memory_space_constraint(h, pltpu.HBM) for h in hidden]
    keep = call(
        shared_keep_body, shape_of(F32, 2, tokens, shard),
        in_specs=[whole(hid_shape)] * 3 + weight_specs(fs, 0, row0, lambda j, s: s[0]),
        out_specs=whole((2, tokens, shard)),
    )(here, *hidden, *shared_w2)
    far = swapped(send, "xl")

    out, grad = call(
        merge_body, (shape_of(BF, tokens, shard),) * 2,
        in_specs=[whole((8 * experts, shard)), whole(keep.shape), whole(far.shape)] + [whole(tall.shape)] * 3,
        out_specs=(act, act),
    )(here, ret.reshape(8 * experts, shard), keep, far, add_hi, add_lo, add_b)
    return out[None], grad[None]


def solution(mesh):
    pipe, expert, tensor = mesh.devices.shape
    fine = Mesh(mesh.devices.reshape(pipe, expert // 2, 2, 2, tensor // 2), ("pipe", "y", "xh", "xl", "core"))
    e, t = ("y", "xh"), ("xl", "core")
    act = P("pipe", e, t)
    table = P(None, "pipe", e, None)

    def step(*args):
        return local(*args)

    step = jax.shard_map(
        step,
        mesh=fine,
        in_specs=(act, act, act, table, table, table, table,
                  P("pipe", e, None, t), P("pipe", e, None, t), P("pipe", e, t, None),
                  P("pipe", None, t), P("pipe", None, t), P("pipe", t, None)),
        out_specs=(act, act),
        check_vma=False,
    )


    return step
```

```python
import jax
import jax.numpy as jnp
from jax import lax
from jax.experimental import pallas as pl
from jax.experimental.pallas import tpu as pltpu
from jax.sharding import Mesh, PartitionSpec as P


BF = jnp.bfloat16
F32 = jnp.float32
I32 = jnp.int32
CAP = 4
PAD = 4 * CAP


def call(body, outs, grid=(1,), in_specs=None, out_specs=None, scratch=(), flops=0, aliases={}):
    spec = pltpu.PrefetchScalarGridSpec(
        num_scalar_prefetch=1, grid=grid, in_specs=in_specs, out_specs=out_specs, scratch_shapes=scratch
    )
    return pl.pallas_call(
        body, grid_spec=spec, out_shape=outs, input_output_aliases=aliases,
        cost_estimate=pl.CostEstimate(flops=flops, transcendentals=0, bytes_accessed=0),
        compiler_params=pltpu.CompilerParams(vmem_limit_bytes=20 * 2**20),
    )


def whole(shape):
    return pl.BlockSpec(shape, lambda j, s: (0,) * len(shape))


hbm = pl.BlockSpec(memory_space=pltpu.HBM)
anywhere = pl.BlockSpec(memory_space=pl.ANY)


def shape_of(dtype, *dims):
    return jax.ShapeDtypeStruct(dims, dtype)


def shifted(block, axis, distance):
    n = lax.axis_size(axis)
    return lax.ppermute(block, axis, [((i - distance) % n, i) for i in range(n)])


def swapped(block, axis):
    return lax.ppermute(block, axis, [(0, 1), (1, 0)])


def dot(a, b):
    return jnp.dot(a, b, preferred_element_type=F32)


def contract_last(left, right):
    return lax.dot_general(left, right, (((1,), (1,)), ((), ())), preferred_element_type=F32)


def make_tables(ids, keep, slot, wq, sel, scale):
    tokens = ids.shape[2]
    row = lax.broadcasted_iota(I32, (tokens, 1), 0)
    arr = (row // CAP) % 4
    slot_id = (row // PAD) * CAP + row % CAP
    want_f = jnp.where(arr == 0, slot_id, -1)
    want_b = jnp.where((arr == 1) | (arr == 2), slot_id, -1)
    hit_f = jnp.zeros((tokens, tokens), F32)
    hit_b = jnp.zeros((tokens, tokens), F32)
    weight = jnp.zeros((tokens, tokens), F32)
    target = jnp.where(keep[...] > 0, ids[...] * CAP + slot[...], -2)
    level = wq[1].astype(F32) * (1.0 / 4096.0)
    for k in range(ids.shape[1]):
        hit_f += jnp.where(target[0, k : k + 1] == want_f, 1.0, 0.0)
        eq = target[1, k : k + 1] == want_b
        hit_b += jnp.where(eq, 1.0, 0.0)
        weight += jnp.where(eq, level[k : k + 1], 0.0)
    sel[0] = hit_f.astype(BF)
    sel[1] = jnp.where(arr == 1, hit_b, 0.0).astype(BF)
    sel[2] = jnp.where(arr == 2, hit_b, 0.0).astype(BF)
    scale[...] = jnp.broadcast_to(jnp.sum(weight, axis=1, keepdims=True), scale.shape)


def adders_body(s, ids, keep, slot, wq, add_hi, add_lo, add_b):
    tokens = ids.shape[2]
    back = add_b.shape[1]
    row = lax.broadcasted_iota(I32, (back, 1), 0)
    dirn = (row // CAP) % 2
    slot_id = (row // 8) * CAP + row % CAP
    back_f = jnp.where(dirn == 0, slot_id, -1)
    back_b = jnp.where(dirn == 1, slot_id, -1)
    hi = jnp.zeros((back, tokens), F32)
    lo = jnp.zeros((back, tokens), F32)
    one = jnp.zeros((back, tokens), F32)
    target = jnp.where(keep[...] > 0, ids[...] * CAP + slot[...], -2)
    level = wq[0]
    top = (level // 64) * 64
    high = top.astype(F32) * (1.0 / 4096.0)
    low = (level - top).astype(F32) * (1.0 / 4096.0)
    for k in range(ids.shape[1]):
        eq = target[0, k : k + 1] == back_f
        hi += jnp.where(eq, high[k : k + 1], 0.0)
        lo += jnp.where(eq, low[k : k + 1], 0.0)
        one += jnp.where(target[1, k : k + 1] == back_b, 1.0, 0.0)
    add_hi[...] = hi.T.astype(BF)
    add_lo[...] = lo.T.astype(BF)
    add_b[...] = one.T.astype(BF)


def parcel_body(s, sel, scale, fwd, saved, cot, out, pair):
    rows = dot(sel[0], fwd[...]) + dot(sel[1], saved[...]) + scale[:, 0:1] * dot(sel[2], cot[...])
    out[...] = rows.astype(BF)
    pair[0] = fwd[...]
    pair[1] = cot[...]


def fan_body(s, got, out):
    n = got.shape[0]
    m = n * 3 // 4
    half = n // 2
    r = lax.broadcasted_iota(I32, (m, n), 0)
    c = lax.broadcasted_iota(I32, (m, n), 1)
    k = r - half
    source = jnp.where(r < half, (r // 8) * PAD + r % 8, (k // CAP) * PAD + 8 + k % CAP)
    rows = dot(jnp.where(c == source, 1.0, 0.0).astype(BF), got[...]).astype(BF)
    for i in range(out.shape[0]):
        out[i] = rows


def run(copies, sems):
    handles = [pltpu.make_async_copy(src, dst, sems.at[i]) for i, (src, dst) in enumerate(copies)]
    for h in handles:
        h.start()

    def wait(lo, hi):
        for h in handles[lo:hi]:
            h.wait()

    return wait


def prep(gs, us, gr, ur, ds, dr, plan, box, sel, scale, hold, ints, sel_v, scale_v, sems, s):
    w = gs.shape[2]
    n = gr.shape[2]
    f = gs.shape[1]
    ready = run([(v, ints.at[i]) for i, v in enumerate(plan)], sems.at[14:18])
    wait = []
    for x in range(2):
        t = 2 * x + 1 - s[1]
        cols = pl.ds(pl.multiple_of(t * f, 128), f)
        h = hold.at[x]
        wait.append(run([
            (gs.at[t], h.at[0:f, 0:w]),
            (us.at[t], h.at[0:f, w : 2 * w]),
            (gr.at[t], h.at[0:f, 2 * w : 2 * w + n]),
            (ur.at[t], h.at[0:f, 2 * w + n : 2 * w + 2 * n]),
            (dr.at[:, cols], h.at[f : f + n]),
            (ds.at[:, cols], h.at[f + n :]),
        ], sems.at[7 * x : 7 * x + 6]))
    ready(0, 4)
    make_tables(*[ints.at[i] for i in range(4)], sel_v, scale_v)
    done = [run([(sel_v, sel), (scale_v, scale)], sems.at[18:20])]
    for x in range(2):
        wait[x](0, 6)
        done.append(run([(hold.at[x], box.at[x])], sems.at[7 * x + 6 : 7 * x + 7]))
    done[0](0, 2)
    done[1](0, 1)
    done[2](0, 1)


def prep_first_body(s, *refs):
    @pl.when(s[2] == 0)
    def _():
        prep(*refs[:6], refs[6:10], *refs[10:], s)


def prep_rest_body(s, *refs):
    @pl.when(s[2] != 0)
    def _():
        prep(*refs[:6], refs[6:10], *refs[13:], s)


def weight_copies(s, order, gate, up, down, box, lane, row, g, u, d):
    f, w = gate.shape[1:]
    gates, ups, downs = [], [], []
    for i, x in enumerate(order):
        t = 2 * x + s[1]
        rows = slice(i * f, i * f + f)
        body = box.at[x, 0:f]
        gates += [(gate.at[t], g.at[rows, 0:w]), (body.at[:, lane : lane + w], g.at[rows, w : 2 * w])]
        ups += [(up.at[t], u.at[rows, 0:w]), (body.at[:, lane + w : lane + 2 * w], u.at[rows, w : 2 * w])]
        downs += [(down.at[:, pl.ds(pl.multiple_of(t * f, 128), f)], d.at[0:w, rows]),
                  (box.at[x, row : row + w], d.at[w : 2 * w, rows])]
    return gates, ups, downs


def joined(mine, other):
    w = mine.shape[1] // 2
    return jnp.concatenate([mine[:, :w] + other[:, w:], mine[:, w:] + other[:, :w]], axis=1)


def pre(wait, n_x, both, cot, g, u, d, acc):
    n = both.shape[0]
    wait(0, n_x + 4)
    acc[0:n] = dot(both[...], g[...])
    wait(n_x + 4, n_x + 8)
    acc[n : 2 * n] = dot(both[...], u[...])
    wait(n_x + 8, n_x + 12)
    acc[2 * n :] = contract_last(cot[...], d[...])


def shared_pre_body(s, fwd, saved, cot, far, far_s, gate, up, down, box, acc, x, g, u, d, sems):
    n, f = fwd.shape
    near, away = slice(0, f), slice(f, 2 * f)
    xs = [(fwd, x.at[0:n, near]), (saved, x.at[n : 2 * n, near]), (cot, x.at[2 * n :, near]),
          (far.at[0], x.at[0:n, away]), (far_s, x.at[n : 2 * n, away]), (far.at[1], x.at[2 * n :, away])]
    ws = weight_copies(s, (s[0], 1 - s[0]), gate, up, down, box, 0, f + gate.shape[2] // 2, g, u, d)
    wait = run(xs + ws[0] + ws[1] + ws[2], sems)
    pre(wait, len(xs), x.at[0 : 2 * n], x.at[2 * n :], g, u, d, acc)


def shared_back(hid, gg, gu, gate, up, down, gate_o, up_o, down_o):
    w = gate.shape[2]
    out = dot(hid[:, :w], down[...]) + dot(hid[:, w:], down_o[0])
    grad = (
        contract_last(gg[:, :w], gate[0]) + contract_last(gg[:, w:], gate_o[0])
        + contract_last(gu[:, :w], up[0]) + contract_last(gu[:, w:], up_o[0])
    )
    return out, grad


def shared_send_body(s, mine, other, gate, up, down, gate_o, up_o, down_o, send, hid_out, gg_out, gu_out):
    n = send.shape[1]
    a_f, a_s, b_f, b_s, dh = [joined(mine[i * n : i * n + n], other[i * n : i * n + n]) for i in range(5)]
    hid = (a_f * jax.nn.sigmoid(a_f) * b_f).astype(BF)
    sg = jax.nn.sigmoid(a_s)
    gg = (dh * b_s * (sg * (1.0 + a_s * (1.0 - sg)))).astype(BF)
    gu = (dh * (a_s * sg)).astype(BF)
    hid_out[...] = hid
    gg_out[...] = gg
    gu_out[...] = gu
    out, grad = shared_back(hid, gg, gu, gate, up, down, gate_o, up_o, down_o)
    send[0] = out.astype(BF)
    send[1] = grad.astype(BF)


def shared_keep_body(s, hid, gg, gu, gate, up, down, gate_o, up_o, down_o, keep):
    keep[0], keep[1] = shared_back(hid[...], gg[...], gu[...], gate, up, down, gate_o, up_o, down_o)


def expert_pre_body(s, got, gate, up, down, box, acc, both, cot, g, u, d, sems):
    n, f = both.shape[0] // 2, got.shape[3]
    m = cot.shape[0] // 2
    xs = []
    for h in range(2):
        for x in range(2):
            cols = slice(x * f, x * f + f)
            xs += [(got.at[h, x, 0:n], both.at[h * n : h * n + n, cols]),
                   (got.at[h, x, n:], cot.at[h * m : h * m + m, cols])]
    w = gate.shape[2]
    ws = weight_copies(s, (0, 1), gate, up, down, box, 4 * w, f, g, u, d)
    wait = run(xs + ws[0] + ws[1] + ws[2], sems)
    pre(wait, len(xs), both, cot, g, u, d, acc)


def expert_post_body(s, mine, other, gate, up, down, gate_o, up_o, down_o, out, hid, gg, gu):
    j = pl.program_id(0)
    n = hid.shape[0]
    m = n // 2

    @pl.when(j == 0)
    def _():
        a = joined(mine[0:n], other[0:n])
        b = joined(mine[n : 2 * n], other[n : 2 * n])
        dh = joined(mine[2 * n : 2 * n + m], other[2 * n : 2 * n + m])
        r = lax.broadcasted_iota(I32, (n, m), 0)
        c = lax.broadcasted_iota(I32, (n, m), 1)
        place = jnp.where(c == (r // 8) * CAP + r % CAP, 1.0, 0.0)
        dh = jnp.dot(place, dh, precision=lax.Precision.HIGHEST, preferred_element_type=F32)
        back = (lax.broadcasted_iota(I32, (n, 1), 0) // CAP) % 2 == 1
        sg = jax.nn.sigmoid(a)
        hid[...] = jnp.where(back, 0.0, a * sg * b).astype(BF)
        gg[...] = jnp.where(back, dh * b * (sg * (1.0 + a * (1.0 - sg))), 0.0).astype(BF)
        gu[...] = jnp.where(back, dh * (a * sg), 0.0).astype(BF)

    g = jnp.concatenate([gate[0], gate_o[0]], axis=1)
    u = jnp.concatenate([up[0], up_o[0]], axis=1)
    d = jnp.concatenate([down[...], down_o[0]], axis=0)
    both = jnp.concatenate([gg[...], gu[...]], axis=1)
    rows = (dot(hid[...], d) + contract_last(both, jnp.concatenate([g, u], axis=1))).astype(BF)
    out[0, 0] = rows[:m]
    out[1, 0] = rows[m:]


def sum_body(s, parts, out):
    p = parts[...].astype(F32)
    out[...] = ((p[0] + p[1]) + (p[2] + p[3])).astype(BF)


def merge_body(s, back, keep, far, add_hi, add_lo, add_b, out, grad):
    rows = back[...]
    out[...] = (keep[0] + far[0].astype(F32) + (dot(add_hi[...], rows) + dot(add_lo[...], rows))).astype(BF)
    grad[...] = (keep[1] + far[1].astype(F32) + dot(add_b[...], rows)).astype(BF)


def local(inputs_prev, cotangent_next, saved_input, expert_ids, keep_mask, slot_pos, weight_q,
          gate_routed, up_routed, down_routed, gate_shared, up_shared, down_shared):
    tokens, shard = inputs_prev.shape[1:]
    experts = lax.axis_size("y")
    here = jnp.stack([lax.axis_index("xl"), lax.axis_index("core"), lax.axis_index("pipe")]).astype(I32)
    saved = saved_input[0]
    gs = gate_shared[0].reshape(4, shard, -1)
    us = up_shared[0].reshape(4, shard, -1)
    ds = down_shared[0]
    gr = gate_routed[0, 0].reshape(4, shard, -1)
    ur = up_routed[0, 0].reshape(4, shard, -1)
    dr = down_routed[0, 0]
    gs, us, ds, gr, ur, dr = [pltpu.with_memory_space_constraint(w, pltpu.HBM) for w in (gs, us, ds, gr, ur, dr)]
    fs = gs.shape[2]
    fe = gr.shape[2]

    fwd = shifted(inputs_prev[0], "pipe", 1)
    cot = shifted(cotangent_next[0], "pipe", -1)
    far_s = swapped(saved, "xl")

    def rows_at(n, which):
        return pl.BlockSpec((1, shard, n), lambda j, s: (which(j, s), 0, 0))

    def cols_at(n, which):
        return pl.BlockSpec((n, shard), lambda j, s: (0, which(j, s)))

    height = shard + fe + fs

    def turned(v):
        return pltpu.with_memory_space_constraint(v[:, 0].transpose(0, 2, 1), pltpu.HBM)

    plan = [turned(v) for v in (expert_ids, keep_mask, slot_pos, weight_q)]
    sq = (tokens, tokens)
    tall = shape_of(BF, tokens, 8 * experts)
    tab = whole((2, expert_ids.shape[3], tokens))
    made = (pltpu.HBM((2, height, shard), BF), pltpu.HBM((3, *sq), BF), pltpu.HBM(sq, F32))
    room = [pltpu.VMEM((2, height, shard), BF), pltpu.VMEM((4, 2, expert_ids.shape[3], tokens), I32),
            pltpu.VMEM((3, *sq), BF), pltpu.VMEM(sq, F32), pltpu.SemaphoreType.DMA((20,))]
    given = (gs, us, gr, ur, ds, dr, *plan)
    first = call(prep_first_body, made, in_specs=[hbm] * 10, out_specs=(hbm,) * 3, scratch=room)(here, *given)
    box, sel, scale = call(
        prep_rest_body, made, in_specs=[hbm] * 13, out_specs=(hbm,) * 3, scratch=room,
        aliases={11: 0, 12: 1, 13: 2},
    )(here, *given, *first)
    box = swapped(box, "core")

    add_hi, add_lo, add_b = call(
        adders_body, (tall, tall, tall), in_specs=[tab] * 4, out_specs=(whole(tall.shape),) * 3,
    )(here, *plan)

    sel, scale = [pltpu.with_memory_space_constraint(v, pltpu.HBM) for v in (sel, scale)]
    act = whole((tokens, shard))
    parcel, pair = call(
        parcel_body, (pltpu.HBM((tokens, shard), BF), pltpu.HBM((2, tokens, shard), BF)),
        in_specs=[whole((3, *sq)), whole(sq)] + [act] * 3, out_specs=(act, whole((2, tokens, shard))),
    )(here, sel, scale, fwd, saved, cot)
    parcel = lax.all_to_all(parcel.reshape(experts, PAD, shard), "y", 0, 0, tiled=True)
    rows = experts * 3 * CAP
    fan = call(
        fan_body, pltpu.HBM((4, rows, shard), BF),
        in_specs=[act], out_specs=whole((4, rows, shard)),
    )(here, parcel.reshape(tokens, shard))
    got = lax.all_to_all(fan, ("xh", "xl"), 0, 0, tiled=True).reshape(2, 2, rows, shard)

    far_fc = swapped(pair, "xl")

    def buffers(w):
        return [pltpu.VMEM((2 * shard, 2 * w), BF)] * 2 + [pltpu.VMEM((2 * w, 2 * shard), BF)]

    def weight_specs(w, lane, row, at):
        mine = lambda j, s: 2 * at(j, s) + s[1]
        return [rows_at(w, mine), rows_at(w, mine), cols_at(w, mine),
                pl.BlockSpec((1, shard, w), lambda j, s: (at(j, s), 0, lane)),
                pl.BlockSpec((1, shard, w), lambda j, s: (at(j, s), 0, lane + 1)),
                pl.BlockSpec((1, w, shard), lambda j, s: (at(j, s), row, 0))]

    straight = lambda j, s: j

    def sems(n):
        return [pltpu.SemaphoreType.DMA((n,))]

    shared_w = (gs, us, ds, box)
    shared_w2 = (gs, us, ds, box, box, box)
    routed_w = (gr, ur, dr, box)
    routed_w2 = (gr, ur, dr, box, box, box)
    z_shape = (5 * tokens, 2 * fs)
    z_s = call(
        shared_pre_body, shape_of(F32, *z_shape),
        in_specs=[anywhere] * 5 + [hbm] * 3 + [anywhere], out_specs=whole(z_shape),
        scratch=[pltpu.VMEM((3 * tokens, 2 * shard), BF)] + buffers(fs) + sems(18),
    )(here, fwd, saved, cot, far_fc, far_s, *shared_w)
    z_s2 = swapped(z_s, "core")

    n_e = 2 * experts * 2 * CAP
    ze_shape = (5 * n_e // 2, 2 * fe)
    z_e = call(
        expert_pre_body, shape_of(F32, *ze_shape),
        in_specs=[anywhere] + [hbm] * 3 + [anywhere], out_specs=whole(ze_shape),
        scratch=[pltpu.VMEM((n_e, 2 * shard), BF), pltpu.VMEM((n_e // 2, 2 * shard), BF)] + buffers(fe) + sems(20),
    )(here, got, *routed_w)
    z_e2 = swapped(z_e, "core")

    ret = call(
        expert_post_body, pltpu.HBM((2, 2, n_e // 2, shard), BF), grid=(2,),
        in_specs=[whole(ze_shape)] * 2 + weight_specs(fe, 2 * fs // fe, shard // fe, straight),
        out_specs=pl.BlockSpec((2, 1, n_e // 2, shard), lambda j, s: (0, j, 0, 0)),
        scratch=[pltpu.VMEM((n_e, 2 * fe), BF)] * 3,
    )(here, z_e, z_e2, *routed_w2)
    ret = lax.all_to_all(ret.reshape(4, n_e // 2, shard), ("xh", "xl"), 0, 0, tiled=True)
    ret = call(
        sum_body, pltpu.HBM((n_e // 2, shard), BF),
        in_specs=[whole((4, n_e // 2, shard))], out_specs=whole((n_e // 2, shard)),
    )(here, ret)
    ret = lax.all_to_all(ret.reshape(experts, 2 * CAP, shard), "y", 0, 0, tiled=True)

    hid_shape = (tokens, 2 * fs)
    row0 = (shard + fe) // fs
    send, *hidden = call(
        shared_send_body, (pltpu.HBM((2, tokens, shard), BF),) + (pltpu.HBM(hid_shape, BF),) * 3,
        in_specs=[whole(z_shape)] * 2 + weight_specs(fs, 0, row0, lambda j, s: 1 - s[0]),
        out_specs=(whole((2, tokens, shard)),) + (whole(hid_shape),) * 3,
    )(here, z_s, z_s2, *shared_w2)
    hidden = [pltpu.with_memory_space_constraint(h, pltpu.HBM) for h in hidden]
    keep = call(
        shared_keep_body, shape_of(F32, 2, tokens, shard),
        in_specs=[whole(hid_shape)] * 3 + weight_specs(fs, 0, row0, lambda j, s: s[0]),
        out_specs=whole((2, tokens, shard)),
    )(here, *hidden, *shared_w2)
    far = swapped(send, "xl")

    out, grad = call(
        merge_body, (shape_of(BF, tokens, shard),) * 2,
        in_specs=[whole((8 * experts, shard)), whole(keep.shape), whole(far.shape)] + [whole(tall.shape)] * 3,
        out_specs=(act, act),
    )(here, ret.reshape(8 * experts, shard), keep, far, add_hi, add_lo, add_b)
    return out[None], grad[None]


def solution(mesh):
    pipe, expert, tensor = mesh.devices.shape
    fine = Mesh(mesh.devices.reshape(pipe, expert // 2, 2, 2, tensor // 2), ("pipe", "y", "xh", "xl", "core"))
    e, t = ("y", "xh"), ("xl", "core")
    act = P("pipe", e, t)
    table = P(None, "pipe", e, None)

    def step(*args):
        return local(*args)

    step = jax.shard_map(
        step,
        mesh=fine,
        in_specs=(act, act, act, table, table, table, table,
                  P("pipe", e, None, t), P("pipe", e, None, t), P("pipe", e, t, None),
                  P("pipe", None, t), P("pipe", None, t), P("pipe", t, None)),
        out_specs=(act, act),
        check_vma=False,
    )


    return step
```
